32 devices in a mesh: chan: 8 (over z, x), blk: 4 (over y, core).
Axes of the slice: x: 2, y: 2, z: 4, core: 2. Of those that a mesh axis runs over, the one named last changes fastest.
Arguments:
- omega: float32 [8, 576, 576], P('chan', 'blk'), may hold values from -0.25 to 0.25
- hamiltonian: float32 [8, 576, 576], P('chan', 'blk'), may hold values from -6 to 6
- pair_occ: float32 [8, 576], P('chan'), may hold values from -1 to 1
- cross_occ: float32 [8, 576], P('chan'), may hold values from -1 to 1
- block_size: int32 [8], P('chan'), may hold values from 288 to 576
- jlabel: int32 [8], replicated, may hold values from 0 to 7
- family: int32 [8], replicated, may hold values from 0 to 3
- sixj: float32 [8, 8], replicated, may hold values from -4 to 4
- column_map: int32 [576], replicated, may hold values from 0 to 575, each once
Outputs:
- evolved: float32 [8, 576, 576], P('chan', 'blk')
The draws below stay inside these ranges and needn't reach their ends.
Inputs may be any that keep to these rules, and one draw needn't show every extreme that they name: `column_map`: a permutation of 0 to 575.
All inputs are finite; a program needn't handle non-finite values.
Results may differ from the reference program's by a relative error of at most 0.0032.
Values may be sent and summed in bfloat16 or wider, within the bound.
No kernel may reach another device: no remote copies, remote signals or barrier semaphores. Data moves between devices by JAX's collectives and lax.ppermute only.
A program may use at most 64 MiB of HBM per device.

```python
import jax
import jax.numpy as jnp
from jax import lax

P_SIZE = 576
FAMILIES = 4
NCHAN = 8
JMAX = 8


def set_ends(result, stream_key, least, top_value):
    longest = result.shape.index(max(result.shape))
    spots = []
    for shift in (0, 1):
        where = [jax.random.randint(jax.random.fold_in(stream_key, axis), (), 0, length) for axis, length in enumerate(result.shape)]
        where[longest] = (where[longest] + shift) % result.shape[longest]
        spots.append(tuple(where))
    return result.at[spots[0]].set(least).at[spots[1]].set(top_value)


def block_scale(rng, shape, split, low, top_value):
    def one(axis_at, blocks):
        draws = jax.random.uniform(jax.random.fold_in(jax.random.fold_in(rng, 6), axis_at), (blocks,), jnp.float32, low / len(split), top_value / len(split))
        return jnp.repeat(jnp.exp(draws), shape[axis_at] // blocks).reshape((-1,) + (1,) * (len(shape) - axis_at - 1))

    loudness = one(*split[0])
    for cut in split[1:]:
        loudness = loudness * one(*cut)
    return loudness


def bell_draw(key, dims, spread, limit, split=(), kind=jnp.bfloat16):
    drawn = spread * jax.random.normal(key, dims, jnp.float32)
    if split:
        drawn = drawn * block_scale(key, dims, split, -0.22, 0.18)
    return jnp.clip(drawn, -limit, limit).astype(kind)


def setup_inputs(seed: int = 0) -> dict:
    splits = jax.random.split(jax.random.key(seed), 10)
    omega = bell_draw(splits[0], (NCHAN, P_SIZE, P_SIZE), P_SIZE ** -0.5, 0.25, ((0, 8), (1, 4)), jnp.float32)
    hamiltonian = bell_draw(splits[1], (NCHAN, P_SIZE, P_SIZE), 1.0, 6.0, ((0, 8), (1, 4)), jnp.float32)
    pair_occ = jnp.clip(jax.random.uniform(splits[2], (NCHAN, P_SIZE), jnp.float32, -1.0, 1.0) * block_scale(splits[2], (NCHAN, P_SIZE), ((0, 8),), -0.4, 0.0), -1.0, 1.0)
    cross_occ = jnp.clip(jax.random.uniform(splits[3], (NCHAN, P_SIZE), jnp.float32, -1.0, 1.0) * block_scale(splits[3], (NCHAN, P_SIZE), ((0, 8),), -0.4, 0.0), -1.0, 1.0)
    block_size = set_ends(jax.random.randint(splits[4], (NCHAN,), P_SIZE // 2, P_SIZE + 1), jax.random.fold_in(splits[4], 1), P_SIZE // 2, P_SIZE).astype(jnp.int32)
    jlabel = set_ends(jax.random.randint(splits[5], (NCHAN,), 0, JMAX), jax.random.fold_in(splits[5], 1), 0, JMAX - 1).astype(jnp.int32)
    family = set_ends(jax.random.randint(splits[6], (NCHAN,), 0, FAMILIES), jax.random.fold_in(splits[6], 1), 0, FAMILIES - 1).astype(jnp.int32)
    sixj = bell_draw(splits[7], (JMAX, JMAX), (NCHAN // FAMILIES) ** -0.5, 4.0, (), jnp.float32)
    column_map = jax.random.permutation(splits[8], P_SIZE).astype(jnp.int32)
    return dict(omega=omega, hamiltonian=hamiltonian, pair_occ=pair_occ, cross_occ=cross_occ, block_size=block_size, jlabel=jlabel, family=family, sixj=sixj, column_map=column_map)


exact_mode = lax.Precision.HIGHEST


def rounded(value):
    return lax.optimization_barrier(value.astype(jnp.bfloat16)).astype(jnp.float32)


def commute(operand_left, operand_right, weights):
    scaled_left = rounded(operand_left * weights[:, None, :])
    scaled_right = rounded(operand_right * weights[:, None, :])
    plain_left = rounded(operand_left)
    plain_right = rounded(operand_right)
    forward_term = jnp.einsum('cik,ckj->cij', scaled_left, plain_right, precision=exact_mode)
    reverse_term = jnp.einsum('cik,ckj->cij', scaled_right, plain_left, precision=exact_mode)
    return forward_term - reverse_term


def reference(omega, hamiltonian, pair_occ, cross_occ, block_size, jlabel, family, sixj, column_map):
    positions = jnp.arange(P_SIZE, dtype=jnp.int32)
    inside_block = (positions[None, :, None] < block_size[:, None, None]) & (positions[None, None, :] < block_size[:, None, None])
    window_mask = inside_block.astype(jnp.float32)
    generator = omega * window_mask
    start_ham = hamiltonian * window_mask
    kindred = (family[:, None] == family[None, :]).astype(jnp.float32)
    mixing = sixj[jlabel[:, None], jlabel[None, :]] * kindred
    inverse_map = jnp.argsort(column_map).astype(jnp.int32)

    def recouple(operand):
        return jnp.einsum('kc,cij->kij', mixing, operand[:, :, column_map], precision=exact_mode)

    def restore(operand):
        return jnp.einsum('ck,cij->kij', mixing, operand, precision=exact_mode)[:, :, inverse_map]

    gen_cross = recouple(generator)
    ham_cross = recouple(start_ham)
    first_pp = commute(generator, start_ham, pair_occ)
    first_cc = commute(gen_cross, ham_cross, cross_occ)
    eta = first_pp + restore(first_cc)
    eta_cross = recouple(eta)
    second = commute(generator, eta, pair_occ) + restore(commute(gen_cross, eta_cross, cross_occ))
    return (start_ham + eta + 0.5 * second) * window_mask
```

```python
import functools

import jax
import jax.numpy as jnp
from jax import lax
from jax.experimental import pallas as pl
from jax.experimental.pallas import tpu as pltpu
from jax.sharding import PartitionSpec as P

exact_mode = lax.Precision.HIGHEST
f32 = jnp.float32
bf16 = jnp.bfloat16
i16 = jnp.int16
LEVELS = 32760.0
STEP = 0.08664339756999316
TINY = 1e-30
HALF = 64


def vmem():
    return pl.BlockSpec(memory_space=pltpu.VMEM)


def smem():
    return pl.BlockSpec(memory_space=pltpu.SMEM)


class Plan:
    def __init__(self, rows, width, chan, blk):
        assert rows % 16 == 0 and width % 128 in (0, HALF) and width >= 128
        self.rows, self.width, self.chan, self.blk = rows, width, chan, blk
        self.full = width // 128
        self.tail = width % 128 != 0
        self.groups = rows // 8
        self.main = self.full * 128
        self.wide = self.main + (128 if self.tail else 0)
        self.packed = 2 * self.main + (128 if self.tail else 0)
        self.tiles = self.groups * self.full + (self.groups // 2 if self.tail else 0)
        self.slots = -(-self.tiles // chan)
        self.pair_rows = 16 * (self.slots + 1)
        self.single_rows = 16 * ((self.slots + 2) // 2)

    def load(self, ref, u):
        if u >= self.tiles:
            return jnp.zeros((8, 128), f32)
        if u < self.groups * self.full:
            g, j = divmod(u, self.full)
            return ref[8 * g : 8 * g + 8, 128 * j : 128 * j + 128]
        v = 16 * (u - self.groups * self.full)
        first = ref[v : v + 8, self.main : self.wide]
        second = pltpu.roll(ref[v + 8 : v + 16, self.main : self.wide], HALF, 1)
        return jnp.where(low_lanes((8, 128)), first, second)

    def store(self, ref, u, tile):
        if u >= self.tiles:
            return
        if u < self.groups * self.full:
            g, j = divmod(u, self.full)
            ref[8 * g : 8 * g + 8, 128 * j : 128 * j + 128] = tile
            return
        v = 16 * (u - self.groups * self.full)
        ref[v : v + 8, self.main : self.wide] = tile
        ref[v + 8 : v + 16, self.main : self.wide] = pltpu.roll(tile, HALF, 1)


def low_lanes(shape):
    return lax.broadcasted_iota(jnp.int32, shape, len(shape) - 1) < HALF


def exponent_of(peak):
    return jnp.floor(jnp.log(jnp.maximum(peak, TINY)) * (1.0 / STEP)) + 1.0


def to_int(value):
    return jnp.round(value).astype(jnp.int32).astype(i16)


def from_int(value):
    return value.astype(jnp.int32).astype(f32)


def pack_pair(plan, first_ref, second_ref, out_ref):
    for chunk in range(plan.chan):
        us = [chunk * plan.slots + p for p in range(plan.slots)]
        values = [jnp.concatenate([plan.load(first_ref, u), plan.load(second_ref, u)], axis=0) for u in us]
        peak = functools.reduce(jnp.maximum, [jnp.abs(v) for v in values])
        e = exponent_of(peak)
        up = jnp.exp(e * -STEP) * LEVELS
        for p, v in enumerate(values):
            out_ref[chunk, 16 * p : 16 * p + 16, :] = to_int(v * up)
        out_ref[chunk, 16 * plan.slots : 16 * plan.slots + 16, :] = to_int(e)


def unpack_pair(plan, in_ref, first_ref, second_ref):
    for chunk in range(plan.chan):
        e = from_int(in_ref[chunk, 16 * plan.slots : 16 * plan.slots + 16, :])
        down = jnp.exp(e * STEP) * (1.0 / LEVELS)
        for p in range(plan.slots):
            u = chunk * plan.slots + p
            if u < plan.tiles:
                v = from_int(in_ref[chunk, 16 * p : 16 * p + 16, :]) * down
                plan.store(first_ref, u, v[0:8])
                plan.store(second_ref, u, v[8:16])


def pack_single(plan, ref, out_ref):
    for chunk in range(plan.chan):
        us = [chunk * plan.slots + p for p in range(plan.slots)]
        values = [plan.load(ref, u) for u in us]
        peak = functools.reduce(jnp.maximum, [jnp.abs(v) for v in values])
        e = exponent_of(peak)
        up = jnp.exp(e * -STEP) * LEVELS
        scaled = [v * up for v in values] + [e]
        if len(scaled) % 2:
            scaled.append(e)
        for p in range(0, len(scaled), 2):
            out_ref[chunk, 8 * p : 8 * p + 16, :] = to_int(jnp.concatenate(scaled[p : p + 2], axis=0))


def single_exponent(plan, tile):
    at = 8 * plan.slots % 16
    return tile[at : at + 8]


def unpack_single(plan, in_ref, ref):
    last = plan.slots // 2
    for chunk in range(plan.chan):
        e = single_exponent(plan, from_int(in_ref[chunk, 16 * last : 16 * last + 16, :]))
        down = jnp.exp(e * STEP) * (1.0 / LEVELS)
        for p in range(0, plan.slots, 2):
            v = from_int(in_ref[chunk, 8 * p : 8 * p + 16, :])
            for q in range(2):
                u = chunk * plan.slots + p + q
                if p + q < plan.slots and u < plan.tiles:
                    plan.store(ref, u, v[8 * q : 8 * q + 8] * down)


def store_packed(plan, first, second, out_ref):
    m = plan.main
    out_ref[:, 0:m] = first[:, 0:m].astype(bf16)
    out_ref[:, m : 2 * m] = second[:, 0:m].astype(bf16)
    if plan.tail:
        a = first[:, m : plan.wide]
        b = pltpu.roll(second[:, m : plan.wide], HALF, 1)
        out_ref[:, 2 * m :] = jnp.where(low_lanes(a.shape), a, b).astype(bf16)


def assemble(plan, pieces, blk_ref, out_ref):
    for s, piece in enumerate(pieces):
        at = pl.multiple_of((blk_ref[0] ^ s) * plan.rows, 16)
        out_ref[pl.ds(at, plan.rows), :] = piece[...]


def dot(a, b):
    return jnp.dot(a, b, preferred_element_type=f32)


def product(plan, left, right_ref, second, main_ref, tail):
    m = plan.main
    at = m if second else 0
    main = dot(left, right_ref[:, at : at + m])
    if not plan.tail:
        return main, None
    last = dot(left, right_ref[:, 2 * m :])
    return main, (pltpu.roll(last, HALF, 1) if second else last)


def commute(plan, left, right_ref, right_second, other_left, other_ref, other_second, out_ref):
    a, a_tail = product(plan, left, right_ref, right_second, None, None)
    b, b_tail = product(plan, other_left, other_ref, other_second, None, None)
    out_ref[:, 0 : plan.main] = a - b
    if plan.tail:
        out_ref[:, plan.main : plan.wide] = a_tail - b_tail


def kernel_enter(plan, omega, ham, occ, size, blk, send, packed, left_gen, left_ham, gen_s, ham_s):
    shape = (plan.rows, plan.width)
    row = lax.broadcasted_iota(jnp.int32, shape, 0) + blk[0] * plan.rows
    col = lax.broadcasted_iota(jnp.int32, shape, 1)
    inside = (row < size[0]) & (col < size[0])
    gen = jnp.where(inside, omega[...], 0.0)
    start = jnp.where(inside, ham[...], 0.0)
    gen_s[:, 0 : plan.width] = gen
    ham_s[:, 0 : plan.width] = start
    left_gen[...] = (gen * occ[...]).astype(bf16)
    left_ham[...] = (start * occ[...]).astype(bf16)
    pack_pair(plan, gen_s, ham_s, send)
    store_packed(plan, gen_s, ham_s, packed)


def kernel_prepare(plan, column_map, occ, select, moved_occ):
    w = plan.width
    rows = lax.broadcasted_iota(jnp.int32, (w, w), 0)
    hot = (rows == column_map[...]).astype(f32).astype(bf16)
    select[...] = hot
    value = occ[...]
    high = value.astype(bf16)
    rest = value - high.astype(f32)
    middle = rest.astype(bf16)
    low = (rest - middle.astype(f32)).astype(bf16)
    total = jnp.zeros((8, w), f32)
    for part in (low, middle, high):
        total = total + lax.dot_general(
            jnp.broadcast_to(part.astype(f32), (8, w)).astype(bf16),
            hot,
            (((1,), (1,)), ((), ())),
            preferred_element_type=f32,
        )
    moved_occ[...] = total[0:1]


def kernel_unpack_cross(plan, recv, packed, gen, ham):
    unpack_pair(plan, recv, gen, ham)
    store_packed(plan, gen, ham, packed)


def moved_left(plan, value_ref, moved_occ, select):
    scaled = (value_ref[:, 0 : plan.width] * moved_occ[...]).astype(bf16)
    return dot(scaled, select[...]).astype(bf16)


def kernel_cross_left(plan, gen, ham, moved_occ, select, left_gen, left_ham):
    left_gen[...] = moved_left(plan, gen, moved_occ, select)
    left_ham[...] = moved_left(plan, ham, moved_occ, select)


def kernel_first_pair(plan, left_gen, left_ham, blk, *refs):
    pieces, (right, first) = refs[: plan.blk], refs[plan.blk :]
    assemble(plan, pieces, blk, right)
    commute(plan, left_gen[...], right, True, left_ham[...], right, False, first)


def kernel_first_cross(plan, left_gen, left_ham, first, blk, *refs):
    pieces, (right, send, cross_s) = refs[: plan.blk], refs[plan.blk :]
    assemble(plan, pieces, blk, right)
    commute(plan, left_gen[...], right, True, left_ham[...], right, False, cross_s)
    pack_pair(plan, cross_s, first, send)


def kernel_unpack_eta(plan, recv, first, occ, packed, eta, cross, left_eta):
    unpack_pair(plan, recv, eta, cross)
    eta[...] = eta[...] + first[...]
    left_eta[...] = (eta[:, 0 : plan.width] * occ[...]).astype(bf16)
    store_packed(plan, cross, eta, packed)


def kernel_eta_left(plan, cross, moved_occ, select, left_cross):
    left_cross[...] = moved_left(plan, cross, moved_occ, select)


def kernel_second_cross(plan, left_gen, left_eta, right_cross, blk, *refs):
    pieces, (right, send, cross_s) = refs[: plan.blk], refs[plan.blk :]
    assemble(plan, pieces, blk, right)
    commute(plan, left_gen[...], right, False, left_eta[...], right_cross, False, cross_s)
    pack_single(plan, cross_s, send)


def kernel_second_pair(plan, left_gen, left_eta, right_eta, right_gen, second):
    commute(plan, left_gen[...], right_eta, True, left_eta[...], right_gen, False, second)


def kernel_finish(plan, recv, ham, eta, second, size, blk, out, back_s):
    unpack_single(plan, recv, back_s)
    w = plan.width
    shape = (plan.rows, w)
    row = lax.broadcasted_iota(jnp.int32, shape, 0) + blk[0] * plan.rows
    col = lax.broadcasted_iota(jnp.int32, shape, 1)
    inside = (row < size[0]) & (col < size[0])
    total = ham[...] + eta[:, 0:w] + 0.5 * (second[:, 0:w] + back_s[:, 0:w])
    out[...] = jnp.where(inside, total, 0.0)


def mixed(mixing, values, transposed):
    n = len(values)
    out = []
    for k in range(n):
        terms = [values[c] * (mixing[c, k] if transposed else mixing[k, c]) for c in range(n)]
        out.append(functools.reduce(jnp.add, terms))
    return out


def both_of(mixing, values):
    restored = mixed(mixing, [v[0:8] for v in values], True)
    crossed = mixed(mixing, [v[8:16] + r for v, r in zip(values, restored)], False)
    return [jnp.concatenate(pair, axis=0) for pair in zip(restored, crossed)]


def kernel_mix(plan, kind, mixing, recv, send, kept):
    n = plan.chan
    slots = plan.slots
    if kind == "back":
        tiles = plan.single_rows // 16
        e_all = [single_exponent(plan, from_int(recv[c, 16 * (slots // 2) : 16 * (slots // 2) + 16, :])) for c in range(n)]
        down = [jnp.exp(e * STEP) * (1.0 / LEVELS) for e in e_all]
        down = [jnp.concatenate([d, d], axis=0) for d in down]
        odd = slots % 2
    else:
        tiles = slots
        down = [jnp.exp(from_int(recv[c, 16 * slots : 16 * slots + 16, :]) * STEP) * (1.0 / LEVELS) for c in range(n)]
    peak = [jnp.zeros((16, 128), f32) for _ in range(n)]
    for p in range(tiles if kind != "back" else (slots + 1) // 2):
        values = [from_int(recv[c, 16 * p : 16 * p + 16, :]) * down[c] for c in range(n)]
        if kind == "cross":
            result = mixed(mixing, values, False)
        elif kind == "both":
            result = both_of(mixing, values)
        else:
            result = mixed(mixing, values, True)
            if odd and p == (slots + 1) // 2 - 1:
                result = [jnp.concatenate([r[0:8], jnp.zeros((8, 128), f32)], axis=0) for r in result]
        for k in range(n):
            kept[k, 16 * p : 16 * p + 16, :] = result[k]
            peak[k] = jnp.maximum(peak[k], jnp.abs(result[k]))
    for k in range(n):
        top = peak[k]
        if kind == "back":
            top = jnp.maximum(top[0:8], top[8:16])
            top = jnp.concatenate([top, top], axis=0)
        e = exponent_of(top)
        up = jnp.exp(e * -STEP) * LEVELS
        if kind != "back":
            for p in range(slots):
                send[k, 16 * p : 16 * p + 16, :] = to_int(kept[k, 16 * p : 16 * p + 16, :] * up)
            send[k, 16 * slots : 16 * slots + 16, :] = to_int(e)
        else:
            for p in range(tiles):
                if 2 * p + 1 < slots:
                    value = kept[k, 16 * p : 16 * p + 16, :] * up
                elif 2 * p < slots:
                    value = jnp.concatenate([kept[k, 16 * p : 16 * p + 8, :] * up[0:8], e[0:8]], axis=0)
                else:
                    value = e
                send[k, 16 * p : 16 * p + 16, :] = to_int(value)


def plain_mix(plan, kind, mixing, recv):
    n, slots = plan.chan, plan.slots

    def mix(spec, value):
        return jnp.einsum(spec, mixing, value, precision=exact_mode, preferred_element_type=f32)

    raw = recv.astype(jnp.int32).astype(f32)
    if kind == "back":
        e = raw[:, 8 * slots : 8 * slots + 8]
        body = raw[:, 0 : 8 * slots].reshape(n, slots, 8, 128)
    else:
        e = raw[:, 16 * slots : 16 * slots + 16]
        body = raw[:, 0 : 16 * slots].reshape(n, slots, 16, 128)
    body = body * (jnp.exp(e * STEP) * (1.0 / LEVELS))[:, None]
    if kind == "cross":
        result = mix("kc,cpsl->kpsl", body)
    elif kind == "both":
        restored = mix("ck,cpsl->kpsl", body[:, :, 0:8])
        crossed = mix("kc,cpsl->kpsl", body[:, :, 8:16] + restored)
        result = jnp.concatenate([restored, crossed], axis=2)
    else:
        result = mix("ck,cpsl->kpsl", body)
    e = exponent_of(jnp.max(jnp.abs(result), axis=1))
    scaled = result * (jnp.exp(e * -STEP) * LEVELS)[:, None]
    out = jnp.concatenate([scaled.reshape(n, -1, 128), e], axis=1)
    out = jnp.pad(out, ((0, 0), (0, recv.shape[1] - out.shape[1]), (0, 0)))
    return to_int(out)


def call(body, plan, outs, specs, scratch=()):
    return pl.pallas_call(
        functools.partial(body, plan),
        out_shape=tuple(jax.ShapeDtypeStruct(s, d) for s, d in outs),
        in_specs=specs,
        out_specs=tuple(vmem() for _ in outs),
        scratch_shapes=tuple(pltpu.VMEM(s, d) for s, d in scratch),
        name=body.__name__,
    )


def mix_call(plan, kind, mixing, recv):
    if plan.chan > 16:
        return plain_mix(plan, kind, mixing, recv)
    rows = recv.shape[1]
    return pl.pallas_call(
        functools.partial(kernel_mix, plan, kind),
        out_shape=jax.ShapeDtypeStruct(recv.shape, i16),
        in_specs=[smem(), vmem()],
        out_specs=vmem(),
        scratch_shapes=(pltpu.VMEM((plan.chan, rows, 128), f32),),
        name="mix_" + kind,
    )(mixing, recv)


def mixing_matrix(jlabel, family, sixj):
    levels = sixj.shape[0]
    one_hot = (jlabel[:, None] == jnp.arange(levels, dtype=jnp.int32)[None, :]).astype(f32)
    picked = jnp.dot(one_hot, sixj, precision=exact_mode, preferred_element_type=f32)
    picked = jnp.dot(picked, one_hot.T, precision=exact_mode, preferred_element_type=f32)
    kindred = (family[:, None] == family[None, :]).astype(f32)
    return picked * kindred


def gather_rows(value, size):
    pieces = {0: value}
    bit = size // 2
    while bit:
        for s, piece in list(pieces.items()):
            pieces[s ^ bit] = lax.ppermute(piece, "blk", [(b, b ^ bit) for b in range(size)])
        bit //= 2
    return [pieces[s] for s in range(size)]


def exchange(value):
    return lax.all_to_all(value, "chan", 0, 0, tiled=True)


def on_device(omega, hamiltonian, pair_occ, cross_occ, block_size, jlabel, family, sixj, column_map):
    channels_here, rows, width = omega.shape
    assert channels_here == 1
    chan, blk = lax.axis_size("chan"), lax.axis_size("blk")
    assert blk & (blk - 1) == 0
    plan = Plan(rows, width, chan, blk)
    omega, ham = omega[0], hamiltonian[0]
    blk_index = lax.axis_index("blk").astype(jnp.int32).reshape(1)
    mixing = mixing_matrix(jlabel, family, sixj)
    pair = ((chan, plan.pair_rows, 128), i16)
    single = ((chan, plan.single_rows, 128), i16)
    packed = ((rows, plan.packed), bf16)
    left = ((rows, width), bf16)
    wide = ((rows, plan.wide), f32)
    right = ((rows * blk, plan.packed), bf16)

    send, pair_rows, left_gen, left_ham = call(
        kernel_enter, plan, [pair, packed, left, left], [vmem(), vmem(), vmem(), smem(), smem()], [wide, wide]
    )(omega, ham, pair_occ, block_size, blk_index)
    select, moved_occ = call(kernel_prepare, plan, [((width, width), bf16), ((1, width), f32)], [vmem(), vmem()])(
        column_map.reshape(1, width), cross_occ
    )
    recv = exchange(send)
    pair_pieces = gather_rows(pair_rows, blk)
    recv = exchange(mix_call(plan, "cross", mixing, recv))
    cross_rows, gen_cross, ham_cross = call(kernel_unpack_cross, plan, [packed, wide, wide], [vmem()])(recv)
    cross_pieces = gather_rows(cross_rows, blk)
    cross_gen_left, cross_ham_left = call(kernel_cross_left, plan, [left, left], [vmem()] * 4)(
        gen_cross, ham_cross, moved_occ, select
    )
    pair_right, first = call(kernel_first_pair, plan, [right, wide], [vmem(), vmem(), smem()] + [vmem()] * blk)(
        left_gen, left_ham, blk_index, *pair_pieces
    )
    cross_right, send = call(
        kernel_first_cross, plan, [right, pair], [vmem(), vmem(), vmem(), smem()] + [vmem()] * blk, [wide]
    )(cross_gen_left, cross_ham_left, first, blk_index, *cross_pieces)
    recv = exchange(mix_call(plan, "both", mixing, exchange(send)))
    eta_rows, eta, eta_cross, left_eta = call(kernel_unpack_eta, plan, [packed, wide, wide, left], [vmem()] * 3)(
        recv, first, pair_occ
    )
    eta_pieces = gather_rows(eta_rows, blk)
    (cross_eta_left,) = call(kernel_eta_left, plan, [left], [vmem()] * 3)(eta_cross, moved_occ, select)
    eta_right, send = call(
        kernel_second_cross, plan, [right, single], [vmem(), vmem(), vmem(), smem()] + [vmem()] * blk, [wide]
    )(cross_gen_left, cross_eta_left, cross_right, blk_index, *eta_pieces)
    (second,) = call(kernel_second_pair, plan, [wide], [vmem()] * 4)(left_gen, left_eta, eta_right, pair_right)
    recv = exchange(mix_call(plan, "back", mixing, exchange(send)))
    (out,) = call(kernel_finish, plan, [((rows, width), f32)], [vmem()] * 4 + [smem(), smem()], [wide])(
        recv, ham, eta, second, block_size, blk_index
    )
    return out[None]


def solution(mesh):
    in_specs = (
        P("chan", "blk", None),
        P("chan", "blk", None),
        P("chan", None),
        P("chan", None),
        P("chan"),
        P(),
        P(),
        P(),
        P(),
    )
    out_specs = P("chan", "blk", None)
    return jax.shard_map(
        on_device, mesh=mesh, in_specs=in_specs, out_specs=out_specs, check_vma=False
    )
```

```python
import functools

import jax
import jax.numpy as jnp
from jax import lax
from jax.experimental import pallas as pl
from jax.experimental.pallas import tpu as pltpu
from jax.sharding import PartitionSpec as P

exact_mode = lax.Precision.HIGHEST
f32 = jnp.float32
bf16 = jnp.bfloat16
i16 = jnp.int16
LEVELS = 32760.0
STEP = 0.08664339756999316
TINY = 1e-30
HALF = 64
UNROLLED = 16
GRANT = 12 << 20


def vmem():
    return pl.BlockSpec(memory_space=pltpu.VMEM)


def smem():
    return pl.BlockSpec(memory_space=pltpu.SMEM)


class Plan:
    def __init__(self, rows, width, chan, blk):
        assert rows % 16 == 0 and width % 128 in (0, HALF) and width >= 128
        self.rows, self.width, self.chan, self.blk = rows, width, chan, blk
        self.full = width // 128
        self.tail = width % 128 != 0
        self.groups = rows // 8
        self.main = self.full * 128
        self.wide = self.main + (128 if self.tail else 0)
        self.packed = 2 * self.main + (128 if self.tail else 0)
        self.tiles = self.groups * self.full + (self.groups // 2 if self.tail else 0)
        self.slots, rest = divmod(self.tiles, chan)
        self.extra = 0
        if rest and chan <= UNROLLED and 8 * rest % chan == 0 and 8 * rest // chan <= 4 and self.slots:
            self.extra = 8 * rest // chan
        elif rest:
            self.slots += 1
        self.pair_rows = 16 * (self.slots + 1)
        self.single_rows = 8 * (self.slots + 1)

    def load(self, ref, u):
        if u >= self.tiles:
            return jnp.zeros((8, 128), f32)
        if u < self.groups * self.full:
            g, j = divmod(u, self.full)
            return ref[8 * g : 8 * g + 8, 128 * j : 128 * j + 128]
        v = 16 * (u - self.groups * self.full)
        first = ref[v : v + 8, self.main : self.wide]
        second = pltpu.roll(ref[v + 8 : v + 16, self.main : self.wide], HALF, 1)
        return jnp.where(low_lanes((8, 128)), first, second)

    def store(self, ref, u, tile):
        if u >= self.tiles:
            return
        if u < self.groups * self.full:
            g, j = divmod(u, self.full)
            ref[8 * g : 8 * g + 8, 128 * j : 128 * j + 128] = tile
            return
        v = 16 * (u - self.groups * self.full)
        ref[v : v + 8, self.main : self.wide] = tile
        ref[v + 8 : v + 16, self.main : self.wide] = pltpu.roll(tile, HALF, 1)


def low_lanes(shape):
    return lax.broadcasted_iota(jnp.int32, shape, len(shape) - 1) < HALF


def sublane():
    return lax.broadcasted_iota(jnp.int32, (8, 128), 0)


def turn(tile, by):
    by %= 8
    return pltpu.roll(tile, by, 0) if by else tile


def lower(tile):
    return jnp.where(sublane() < 4, tile, turn(tile, 4))


def spread(tile):
    other = turn(tile, 4)
    low = sublane() < 4
    return jnp.concatenate([jnp.where(low, tile, other), jnp.where(low, other, tile)], axis=0)


def exponent_of(peak):
    return jnp.floor(jnp.log(jnp.maximum(peak, TINY)) * (1.0 / STEP)) + 1.0


def scale_up(e):
    return jnp.exp(e * -STEP) * LEVELS


def scale_down(e):
    return jnp.exp(e * STEP) * (1.0 / LEVELS)


def to_int(value):
    return jnp.round(value).astype(jnp.int32).astype(i16)


def from_int(value):
    return value.astype(jnp.int32).astype(f32)


def largest(values):
    return functools.reduce(jnp.maximum, [jnp.abs(v) for v in values])


def take_extra(plan, ref, chunk, at):
    out = jnp.zeros((8, 128), f32)
    for m in range(plan.extra):
        tile, row = divmod(chunk * plan.extra + m, 8)
        value = plan.load(ref, plan.chan * plan.slots + tile)
        out = jnp.where(sublane() == at + m, turn(value, at + m - row), out)
    return out


def put_extra(plan, ref, extras, at):
    if not plan.extra:
        return
    tiles = [jnp.zeros((8, 128), f32) for _ in range(plan.chan * plan.extra // 8)]
    for chunk, value in enumerate(extras):
        for m in range(plan.extra):
            tile, row = divmod(chunk * plan.extra + m, 8)
            tiles[tile] = jnp.where(sublane() == row, turn(value, row - at - m), tiles[tile])
    for tile, value in enumerate(tiles):
        plan.store(ref, plan.chan * plan.slots + tile, value)


def encode_pair(plan, values, extra, write):
    peak = largest(values)
    first = jnp.maximum(peak[0:8], turn(peak[0:8], 4))
    second = jnp.maximum(peak[8:16], turn(peak[8:16], 4))
    peak = jnp.maximum(jnp.where(sublane() < 4, first, second), jnp.abs(extra))
    e = exponent_of(peak)
    up = scale_up(e)
    both = spread(up)
    for p, v in enumerate(values):
        write(p, to_int(v * both))
    write(plan.slots, to_int(jnp.concatenate([e, extra * up], axis=0)))


def pair_scale(plan, in_ref, chunk):
    last = from_int(in_ref[chunk, 16 * plan.slots : 16 * plan.slots + 16, :])
    down = scale_down(last[0:8])
    return spread(down), last[8:16] * down


def write_pair(out_ref, chunk):
    def write(p, tile):
        out_ref[chunk, 16 * p : 16 * p + 16, :] = tile

    return write


def pack_pair(plan, first_ref, second_ref, out_ref):
    for chunk in range(plan.chan):
        us = [chunk * plan.slots + p for p in range(plan.slots)]
        values = [jnp.concatenate([plan.load(first_ref, u), plan.load(second_ref, u)], axis=0) for u in us]
        extra = take_extra(plan, first_ref, chunk, 0) + take_extra(plan, second_ref, chunk, 4)
        encode_pair(plan, values, extra, write_pair(out_ref, chunk))


def unpack_pair(plan, in_ref, first_ref, second_ref):
    extras = []
    for chunk in range(plan.chan):
        down, extra = pair_scale(plan, in_ref, chunk)
        extras.append(extra)
        for p in range(plan.slots):
            u = chunk * plan.slots + p
            if u < plan.tiles:
                v = from_int(in_ref[chunk, 16 * p : 16 * p + 16, :]) * down
                plan.store(first_ref, u, v[0:8])
                plan.store(second_ref, u, v[8:16])
    put_extra(plan, first_ref, extras, 0)
    put_extra(plan, second_ref, extras, 4)


def encode_single(plan, values, extra, out_ref, chunk):
    peak = jnp.maximum(largest(values), jnp.abs(extra))
    e = exponent_of(jnp.maximum(peak, turn(peak, 4)))
    up = scale_up(e)
    scaled = [v * up for v in values] + [jnp.where(sublane() < 4, e, extra * up)]
    for p in range(0, len(scaled), 2):
        part = scaled[p : p + 2]
        out_ref[chunk, 8 * p : 8 * (p + len(part)), :] = to_int(jnp.concatenate(part, axis=0))


def decode_single(plan, in_ref, chunk):
    rows = from_int(in_ref[chunk, 8 * plan.slots : 8 * plan.slots + 8, :])
    down = scale_down(lower(rows))
    values = []
    for p in range(plan.slots):
        values.append(from_int(in_ref[chunk, 8 * p : 8 * p + 8, :]) * down)
    return values, rows * down


def pack_single(plan, ref, out_ref):
    for chunk in range(plan.chan):
        values = [plan.load(ref, chunk * plan.slots + p) for p in range(plan.slots)]
        encode_single(plan, values, take_extra(plan, ref, chunk, 4), out_ref, chunk)


def unpack_single(plan, in_ref, ref):
    extras = []
    for chunk in range(plan.chan):
        values, extra = decode_single(plan, in_ref, chunk)
        extras.append(extra)
        for p, value in enumerate(values):
            plan.store(ref, chunk * plan.slots + p, value)
    put_extra(plan, ref, extras, 4)


def store_packed(plan, first, second, out_ref):
    m = plan.main
    out_ref[:, 0:m] = first[:, 0:m].astype(bf16)
    out_ref[:, m : 2 * m] = second[:, 0:m].astype(bf16)
    if plan.tail:
        a = first[:, m : plan.wide]
        b = pltpu.roll(second[:, m : plan.wide], HALF, 1)
        out_ref[:, 2 * m :] = jnp.where(low_lanes(a.shape), a, b).astype(bf16)


def assemble(plan, pieces, blk_ref, out_ref):
    for s, piece in enumerate(pieces):
        at = pl.multiple_of((blk_ref[0] ^ s) * plan.rows, 16)
        out_ref[pl.ds(at, plan.rows), :] = piece[...]


def dot(a, b):
    return jnp.dot(a, b, preferred_element_type=f32)


def product(plan, left, right_ref, second, main_ref, tail):
    m = plan.main
    at = m if second else 0
    main = dot(left, right_ref[:, at : at + m])
    if not plan.tail:
        return main, None
    last = dot(left, right_ref[:, 2 * m :])
    return main, (pltpu.roll(last, HALF, 1) if second else last)


def commute(plan, left, right_ref, right_second, other_left, other_ref, other_second, out_ref):
    a, a_tail = product(plan, left, right_ref, right_second, None, None)
    b, b_tail = product(plan, other_left, other_ref, other_second, None, None)
    out_ref[:, 0 : plan.main] = a - b
    if plan.tail:
        out_ref[:, plan.main : plan.wide] = a_tail - b_tail


def inside_of(plan, size, blk):
    shape = (plan.rows, plan.width)
    row = lax.broadcasted_iota(jnp.int32, shape, 0) + blk[0] * plan.rows
    col = lax.broadcasted_iota(jnp.int32, shape, 1)
    return (row < size[0]) & (col < size[0])


def kernel_enter(plan, omega, ham, occ, size, blk, send, packed, left_gen, left_ham, gen_s, ham_s):
    inside = inside_of(plan, size, blk)
    gen = jnp.where(inside, omega[...], 0.0)
    start = jnp.where(inside, ham[...], 0.0)
    gen_s[:, 0 : plan.width] = gen
    ham_s[:, 0 : plan.width] = start
    left_gen[...] = (gen * occ[...]).astype(bf16)
    left_ham[...] = (start * occ[...]).astype(bf16)
    pack_pair(plan, gen_s, ham_s, send)
    store_packed(plan, gen_s, ham_s, packed)


def kernel_prepare(plan, column_map, occ, select, moved_occ):
    w = plan.width
    rows = lax.broadcasted_iota(jnp.int32, (w, w), 0)
    hot = (rows == column_map[...]).astype(f32).astype(bf16)
    select[...] = hot
    value = occ[...]
    high = value.astype(bf16)
    rest = value - high.astype(f32)
    middle = rest.astype(bf16)
    low = (rest - middle.astype(f32)).astype(bf16)
    total = jnp.zeros((8, w), f32)
    for part in (low, middle, high):
        total = total + lax.dot_general(
            jnp.broadcast_to(part.astype(f32), (8, w)).astype(bf16),
            hot,
            (((1,), (1,)), ((), ())),
            preferred_element_type=f32,
        )
    moved_occ[...] = total[0:1]


def kernel_unpack_cross(plan, recv, moved_occ, packed, scaled_gen, scaled_ham, gen, ham):
    unpack_pair(plan, recv, gen, ham)
    store_packed(plan, gen, ham, packed)
    scaled_gen[...] = (gen[:, 0 : plan.width] * moved_occ[...]).astype(bf16)
    scaled_ham[...] = (ham[:, 0 : plan.width] * moved_occ[...]).astype(bf16)


def keep_first(plan, right, kept):
    m = plan.main
    kept[:, 0:m] = right[:, 0:m]
    if plan.tail:
        kept[:, m:] = right[:, 2 * m :]


def kernel_cross_left(plan, scaled_gen, scaled_ham, select, cross_gen, cross_ham):
    cross_gen[...] = dot(scaled_gen[...], select[...]).astype(bf16)
    cross_ham[...] = dot(scaled_ham[...], select[...]).astype(bf16)


def kernel_first_pair(plan, left_gen, left_ham, blk, *refs):
    pieces, (right_gen, first, right) = refs[: plan.blk], refs[plan.blk :]
    assemble(plan, pieces, blk, right)
    commute(plan, left_gen[...], right, True, left_ham[...], right, False, first)
    keep_first(plan, right, right_gen)


def kernel_first_cross(plan, left_gen, left_ham, first, blk, *refs):
    pieces, (right_gen, send, right, cross_s) = refs[: plan.blk], refs[plan.blk :]
    assemble(plan, pieces, blk, right)
    commute(plan, left_gen[...], right, True, left_ham[...], right, False, cross_s)
    keep_first(plan, right, right_gen)
    pack_pair(plan, cross_s, first, send)


def kernel_unpack_eta(plan, recv, first, occ, moved_occ, cross_rows, eta_rows, eta, left_eta, scaled_cross, cross):
    w = plan.width
    unpack_pair(plan, recv, eta, cross)
    eta[...] = eta[...] + first[...]
    cross_rows[...] = cross[:, 0:w].astype(bf16)
    eta_rows[...] = eta[:, 0:w].astype(bf16)
    left_eta[...] = (eta[:, 0:w] * occ[...]).astype(bf16)
    scaled_cross[...] = (cross[:, 0:w] * moved_occ[...]).astype(bf16)


def kernel_eta_left(plan, scaled_cross, select, left_cross):
    left_cross[...] = dot(scaled_cross[...], select[...]).astype(bf16)


def kernel_second_cross(plan, left_gen, left_eta, right_gen, blk, *refs):
    pieces, (send, right, cross_s) = refs[: plan.blk], refs[plan.blk :]
    w = plan.width
    assemble(plan, pieces, blk, right)
    cross_s[:, 0:w] = dot(left_gen[...], right[...]) - dot(left_eta[...], right_gen[:, 0:w])
    pack_single(plan, cross_s, send)


def kernel_second_pair(plan, left_gen, left_eta, right_gen, blk, *refs):
    pieces, (second, right) = refs[: plan.blk], refs[plan.blk :]
    assemble(plan, pieces, blk, right)
    second[...] = dot(left_gen[...], right[...]) - dot(left_eta[...], right_gen[:, 0 : plan.width])


def kernel_finish(plan, recv, ham, eta, second, size, blk, out, back_s):
    unpack_single(plan, recv, back_s)
    w = plan.width
    total = ham[...] + eta[:, 0:w] + 0.5 * (second[...] + back_s[:, 0:w])
    out[...] = jnp.where(inside_of(plan, size, blk), total, 0.0)


def mixed(mixing, values, transposed):
    n = len(values)
    out = []
    for k in range(n):
        terms = [values[c] * (mixing[c, k] if transposed else mixing[k, c]) for c in range(n)]
        out.append(functools.reduce(jnp.add, terms))
    return out


def both_of(mixing, first, second):
    restored = mixed(mixing, first, True)
    crossed = mixed(mixing, [v + r for v, r in zip(second, restored)], False)
    return restored, crossed


def kernel_mix_pair(plan, both, mixing, recv, send, kept):
    n = plan.chan
    scales = [pair_scale(plan, recv, c) for c in range(n)]
    extra = [s[1] for s in scales]
    if both:
        restored, crossed = both_of(mixing, extra, [turn(x, 4) for x in extra])
        extra = [jnp.where(sublane() < 4, r, turn(x, 4)) for r, x in zip(restored, crossed)]
    else:
        extra = mixed(mixing, extra, False)
    for p in range(plan.slots):
        values = [from_int(recv[c, 16 * p : 16 * p + 16, :]) * scales[c][0] for c in range(n)]
        if both:
            pairs = zip(*both_of(mixing, [v[0:8] for v in values], [v[8:16] for v in values]))
            result = [jnp.concatenate(pair, axis=0) for pair in pairs]
        else:
            result = mixed(mixing, values, False)
        for k in range(n):
            kept[k, 16 * p : 16 * p + 16, :] = result[k]
    for k in range(n):
        values = [kept[k, 16 * p : 16 * p + 16, :] for p in range(plan.slots)]
        encode_pair(plan, values, extra[k], write_pair(send, k))


def kernel_mix_single(plan, both, mixing, recv, send, kept):
    n = plan.chan
    downs, extra = [], []
    for c in range(n):
        rows = from_int(recv[c, 8 * plan.slots : 8 * plan.slots + 8, :])
        downs.append(scale_down(lower(rows)))
        extra.append(rows * downs[c])
    extra = mixed(mixing, extra, True)
    for p in range(plan.slots):
        result = mixed(mixing, [from_int(recv[c, 8 * p : 8 * p + 8, :]) * downs[c] for c in range(n)], True)
        for k in range(n):
            kept[k, 8 * p : 8 * p + 8, :] = result[k]
    for k in range(n):
        values = [kept[k, 8 * p : 8 * p + 8, :] for p in range(plan.slots)]
        encode_single(plan, values, extra[k], send, k)


def plain_mix(plan, kind, mixing, recv):
    n, slots = plan.chan, plan.slots

    def mix(spec, value):
        return jnp.einsum(spec, mixing, value, precision=exact_mode, preferred_element_type=f32)

    def spread_rows(e):
        if kind == "back":
            return jnp.concatenate([e[:, 0:4]] * 2, axis=1)
        return jnp.concatenate([e[:, 0:4]] * 2 + [e[:, 4:8]] * 2, axis=1)

    raw = recv.astype(jnp.int32).astype(f32)
    high = 8 if kind == "back" else 16
    e = raw[:, high * slots : high * slots + 8]
    body = raw[:, 0 : high * slots].reshape(n, slots, high, 128) * scale_down(spread_rows(e))[:, None]
    if kind == "cross":
        result = mix("kc,cpsl->kpsl", body)
    elif kind == "both":
        restored = mix("ck,cpsl->kpsl", body[:, :, 0:8])
        crossed = mix("kc,cpsl->kpsl", body[:, :, 8:16] + restored)
        result = jnp.concatenate([restored, crossed], axis=2)
    else:
        result = mix("ck,cpsl->kpsl", body)
    peak = jnp.max(jnp.abs(result), axis=1)
    peak = jnp.max(peak.reshape(n, high // 8, 2, 4, 128), axis=2).reshape(n, high // 2, 128)
    e = exponent_of(peak)
    scaled = result * scale_up(spread_rows(e))[:, None]
    out = jnp.concatenate([scaled.reshape(n, -1, 128), e], axis=1)
    out = jnp.pad(out, ((0, 0), (0, recv.shape[1] - out.shape[1]), (0, 0)))
    return to_int(out)


def near(value):
    return pltpu.with_memory_space_constraint(value, pltpu.VMEM)


def call(body, plan, outs, specs, scratch=(), flops=0, final=False):
    def run(*operands):
        places = {"v": pltpu.VMEM, "h": pltpu.HBM}
        placed = [
            pltpu.with_memory_space_constraint(x, places[s]) if s in places else x
            for x, s in zip(operands, specs, strict=True)
        ]
        return pl.pallas_call(
            functools.partial(body, plan),
            out_shape=tuple((jax.ShapeDtypeStruct if final else pltpu.VMEM)(s, d) for s, d in outs),
            in_specs=[smem() if s == "s" else vmem() for s in specs],
            out_specs=tuple(vmem() for _ in outs),
            scratch_shapes=tuple(pltpu.VMEM(s, d) for s, d in scratch),
            name=body.__name__,
            cost_estimate=pl.CostEstimate(flops=flops or plan.rows * plan.width * 60000, transcendentals=0, bytes_accessed=0),
            compiler_params=pltpu.CompilerParams(vmem_limit_bytes=GRANT),
        )(*placed)

    return run


def mix_call(plan, kind, mixing, recv):
    if plan.chan > UNROLLED:
        return plain_mix(plan, kind, mixing, recv)
    body = kernel_mix_single if kind == "back" else kernel_mix_pair
    return pl.pallas_call(
        functools.partial(body, plan, kind == "both"),
        out_shape=pltpu.VMEM(recv.shape, i16),
        in_specs=[smem(), vmem()],
        out_specs=vmem(),
        scratch_shapes=(pltpu.VMEM((plan.chan, recv.shape[1], 128), f32),),
        name="mix_" + kind,
        compiler_params=pltpu.CompilerParams(vmem_limit_bytes=GRANT),
    )(mixing, near(recv))


def mixing_matrix(jlabel, family, sixj):
    levels = sixj.shape[0]
    one_hot = (jlabel[:, None] == jnp.arange(levels, dtype=jnp.int32)[None, :]).astype(f32)
    picked = jnp.dot(one_hot, sixj, precision=exact_mode, preferred_element_type=f32)
    picked = jnp.dot(picked, one_hot.T, precision=exact_mode, preferred_element_type=f32)
    kindred = (family[:, None] == family[None, :]).astype(f32)
    return picked * kindred


def swap(value, size, bits):
    return lax.ppermute(value, "blk", [(b, b ^ bits) for b in range(size)])


def far_rows(value, size):
    return swap(value, size, size // 2) if size > 1 else None


def near_rows(value, far, size):
    pieces = {0: value}
    bit = size // 2
    while bit:
        for s, piece in list(pieces.items()):
            pieces[s ^ bit] = far if bit == size // 2 and s == 0 else swap(piece, size, bit)
        bit //= 2
    return [pieces[s] for s in range(size)]


def exchange(value):
    return lax.all_to_all(value, "chan", 0, 0, tiled=True)


def on_device(omega, hamiltonian, pair_occ, cross_occ, block_size, jlabel, family, sixj, column_map):
    channels_here, rows, width = omega.shape
    assert channels_here == 1
    chan, blk = lax.axis_size("chan"), lax.axis_size("blk")
    assert blk & (blk - 1) == 0
    plan = Plan(rows, width, chan, blk)
    omega, ham = omega[0], hamiltonian[0]
    blk_index = lax.axis_index("blk").astype(jnp.int32).reshape(1)
    pair = ((chan, plan.pair_rows, 128), i16)
    single = ((chan, plan.single_rows, 128), i16)
    packed = ((rows, plan.packed), bf16)
    left = ((rows, width), bf16)
    plain = ((rows, width), f32)
    wide = ((rows, plan.wide), f32)
    right = ((rows * blk, plan.packed), bf16)
    right_kept = ((rows * blk, plan.wide), bf16)
    right_one = ((rows * blk, width), bf16)

    send, pair_rows, left_gen, left_ham = call(
        kernel_enter, plan, [pair, packed, left, left], "hhhss", [wide, wide]
    )(omega, ham, pair_occ, block_size, blk_index)
    select, moved_occ = call(kernel_prepare, plan, [((width, width), bf16), ((1, width), f32)], "vv")(
        column_map.reshape(1, width), cross_occ
    )
    mixing = mixing_matrix(jlabel, family, sixj)
    pair_far = far_rows(pair_rows, blk)
    recv = exchange(send)
    recv, mixing, select, moved_occ, pair_far = lax.optimization_barrier((recv, mixing, select, moved_occ, pair_far))
    pair_pieces = near_rows(pair_rows, pair_far, blk)
    recv = exchange(mix_call(plan, "cross", mixing, recv))
    pair_right, first = call(kernel_first_pair, plan, [right_kept, wide], "vvs" + "v" * blk, [right])(
        left_gen, left_ham, blk_index, *pair_pieces
    )
    recv, pair_right, first = lax.optimization_barrier((recv, pair_right, first))
    cross_rows, scaled_gen, scaled_ham = call(
        kernel_unpack_cross, plan, [packed, left, left], "vv", [wide, wide]
    )(recv, moved_occ)
    cross_pieces = near_rows(cross_rows, far_rows(cross_rows, blk), blk)
    cross_gen_left, cross_ham_left = call(kernel_cross_left, plan, [left, left], "vvv")(scaled_gen, scaled_ham, select)
    cross_right, send = call(
        kernel_first_cross, plan, [right_kept, pair], "vvvs" + "v" * blk, [right, wide]
    )(cross_gen_left, cross_ham_left, first, blk_index, *cross_pieces)
    recv = exchange(mix_call(plan, "both", mixing, exchange(send)))
    cross_rows, eta_rows, eta, left_eta, scaled_cross = call(
        kernel_unpack_eta, plan, [left, left, wide, left, left], "vvvv", [wide]
    )(recv, first, pair_occ, moved_occ)
    cross_far = far_rows(cross_rows, blk)
    eta_far = far_rows(eta_rows, blk)
    cross_pieces = near_rows(cross_rows, cross_far, blk)
    (cross_eta_left,) = call(kernel_eta_left, plan, [left], "vv")(scaled_cross, select)
    (send,) = call(kernel_second_cross, plan, [single], "vvvs" + "v" * blk, [right_one, wide])(
        cross_gen_left, cross_eta_left, cross_right, blk_index, *cross_pieces
    )
    send, eta_far = lax.optimization_barrier((send, eta_far))
    recv = exchange(send)
    eta_pieces = near_rows(eta_rows, eta_far, blk)
    (second,) = call(kernel_second_pair, plan, [plain], "vvvs" + "v" * blk, [right_one])(
        left_gen, left_eta, pair_right, blk_index, *eta_pieces
    )
    recv, second = lax.optimization_barrier((recv, second))
    recv = exchange(mix_call(plan, "back", mixing, recv))
    (out,) = call(kernel_finish, plan, [plain], "vhvvss", [wide], final=True)(
        recv, ham, eta, second, block_size, blk_index
    )
    return out[None]


def solution(mesh):
    in_specs = (
        P("chan", "blk", None),
        P("chan", "blk", None),
        P("chan", None),
        P("chan", None),
        P("chan"),
        P(),
        P(),
        P(),
        P(),
    )
    out_specs = P("chan", "blk", None)
    return jax.shard_map(
        on_device, mesh=mesh, in_specs=in_specs, out_specs=out_specs, check_vma=False
    )
```

```python
import functools

import jax
import jax.numpy as jnp
from jax import lax
from jax.experimental import pallas as pl
from jax.experimental.pallas import tpu as pltpu
from jax.sharding import PartitionSpec as P

exact_mode = lax.Precision.HIGHEST
f32 = jnp.float32
bf16 = jnp.bfloat16
i16 = jnp.int16
LEVELS = 32760.0
STEP = 0.08664339756999316
TINY = 1e-30
HALF = 64
UNROLLED = 16
GRANT = 12 << 20


def vmem():
    return pl.BlockSpec(memory_space=pltpu.VMEM)


def smem():
    return pl.BlockSpec(memory_space=pltpu.SMEM)


class Plan:
    def __init__(self, rows, width, chan, blk):
        assert rows % 16 == 0 and width % 128 in (0, HALF) and width >= 128
        self.rows, self.width, self.chan, self.blk = rows, width, chan, blk
        self.full = width // 128
        self.tail = width % 128 != 0
        self.groups = rows // 8
        self.main = self.full * 128
        self.wide = self.main + (128 if self.tail else 0)
        self.packed = 2 * self.main + (128 if self.tail else 0)
        self.tiles = self.groups * self.full + (self.groups // 2 if self.tail else 0)
        self.slots, rest = divmod(self.tiles, chan)
        self.extra = 0
        if rest and chan <= UNROLLED and 8 * rest % chan == 0 and 8 * rest // chan <= 4 and self.slots:
            self.extra = 8 * rest // chan
        elif rest:
            self.slots += 1
        self.pair_rows = 16 * (self.slots + 1)
        self.single_rows = 8 * (self.slots + 1)

    def load(self, ref, u):
        if u >= self.tiles:
            return jnp.zeros((8, 128), f32)
        if u < self.groups * self.full:
            g, j = divmod(u, self.full)
            return ref[8 * g : 8 * g + 8, 128 * j : 128 * j + 128]
        v = 16 * (u - self.groups * self.full)
        first = ref[v : v + 8, self.main : self.wide]
        second = pltpu.roll(ref[v + 8 : v + 16, self.main : self.wide], HALF, 1)
        return jnp.where(low_lanes((8, 128)), first, second)

    def store(self, ref, u, tile):
        if u >= self.tiles:
            return
        if u < self.groups * self.full:
            g, j = divmod(u, self.full)
            ref[8 * g : 8 * g + 8, 128 * j : 128 * j + 128] = tile
            return
        v = 16 * (u - self.groups * self.full)
        ref[v : v + 8, self.main : self.wide] = tile
        ref[v + 8 : v + 16, self.main : self.wide] = pltpu.roll(tile, HALF, 1)


def low_lanes(shape):
    return lax.broadcasted_iota(jnp.int32, shape, len(shape) - 1) < HALF


def sublane():
    return lax.broadcasted_iota(jnp.int32, (8, 128), 0)


def turn(tile, by):
    by %= 8
    return pltpu.roll(tile, by, 0) if by else tile


def lower(tile):
    return jnp.where(sublane() < 4, tile, turn(tile, 4))


def spread(tile):
    other = turn(tile, 4)
    low = sublane() < 4
    return jnp.concatenate([jnp.where(low, tile, other), jnp.where(low, other, tile)], axis=0)


def exponent_of(peak):
    return jnp.floor(jnp.log(jnp.maximum(peak, TINY)) * (1.0 / STEP)) + 1.0


def scale_up(e):
    return jnp.exp(e * -STEP) * LEVELS


def scale_down(e):
    return jnp.exp(e * STEP) * (1.0 / LEVELS)


def to_int(value):
    return jnp.round(value).astype(jnp.int32).astype(i16)


def from_int(value):
    return value.astype(jnp.int32).astype(f32)


def largest(values):
    return functools.reduce(jnp.maximum, [jnp.abs(v) for v in values])


def take_extra(plan, ref, chunk, at):
    out = jnp.zeros((8, 128), f32)
    for m in range(plan.extra):
        tile, row = divmod(chunk * plan.extra + m, 8)
        value = plan.load(ref, plan.chan * plan.slots + tile)
        out = jnp.where(sublane() == at + m, turn(value, at + m - row), out)
    return out


def put_extra(plan, ref, extras, at):
    if not plan.extra:
        return
    tiles = [jnp.zeros((8, 128), f32) for _ in range(plan.chan * plan.extra // 8)]
    for chunk, value in enumerate(extras):
        for m in range(plan.extra):
            tile, row = divmod(chunk * plan.extra + m, 8)
            tiles[tile] = jnp.where(sublane() == row, turn(value, row - at - m), tiles[tile])
    for tile, value in enumerate(tiles):
        plan.store(ref, plan.chan * plan.slots + tile, value)


def encode_pair(plan, values, extra, write):
    peak = largest(values)
    first = jnp.maximum(peak[0:8], turn(peak[0:8], 4))
    second = jnp.maximum(peak[8:16], turn(peak[8:16], 4))
    peak = jnp.maximum(jnp.where(sublane() < 4, first, second), jnp.abs(extra))
    e = exponent_of(peak)
    up = scale_up(e)
    both = spread(up)
    for p, v in enumerate(values):
        write(p, to_int(v * both))
    write(plan.slots, to_int(jnp.concatenate([e, extra * up], axis=0)))


def pair_scale(plan, in_ref, chunk):
    last = from_int(in_ref[chunk, 16 * plan.slots : 16 * plan.slots + 16, :])
    down = scale_down(last[0:8])
    return spread(down), last[8:16] * down


def write_pair(out_ref, chunk):
    def write(p, tile):
        out_ref[chunk, 16 * p : 16 * p + 16, :] = tile

    return write


def pack_pair(plan, first_ref, second_ref, out_ref):
    for chunk in range(plan.chan):
        us = [chunk * plan.slots + p for p in range(plan.slots)]
        values = [jnp.concatenate([plan.load(first_ref, u), plan.load(second_ref, u)], axis=0) for u in us]
        extra = take_extra(plan, first_ref, chunk, 0) + take_extra(plan, second_ref, chunk, 4)
        encode_pair(plan, values, extra, write_pair(out_ref, chunk))


def unpack_pair(plan, in_ref, first_ref, second_ref):
    extras = []
    for chunk in range(plan.chan):
        down, extra = pair_scale(plan, in_ref, chunk)
        extras.append(extra)
        for p in range(plan.slots):
            u = chunk * plan.slots + p
            if u < plan.tiles:
                v = from_int(in_ref[chunk, 16 * p : 16 * p + 16, :]) * down
                plan.store(first_ref, u, v[0:8])
                plan.store(second_ref, u, v[8:16])
    put_extra(plan, first_ref, extras, 0)
    put_extra(plan, second_ref, extras, 4)


def encode_single(values, extra, out_ref, chunk):
    peak = jnp.maximum(largest(values), jnp.abs(extra))
    e = exponent_of(jnp.maximum(peak, turn(peak, 4)))
    up = scale_up(e)
    scaled = [v * up for v in values] + [jnp.where(sublane() < 4, e, extra * up)]
    for p in range(0, len(scaled), 2):
        part = scaled[p : p + 2]
        out_ref[chunk, 8 * p : 8 * (p + len(part)), :] = to_int(jnp.concatenate(part, axis=0))


def single_tiles(plan, in_ref, chunk, scale):
    values = []
    for p in range(0, plan.slots, 2):
        n = min(2, plan.slots - p)
        rows = from_int(in_ref[chunk, 8 * p : 8 * (p + n), :])
        values += [rows[8 * q : 8 * q + 8] * scale for q in range(n)]
    return values


def single_scale(plan, in_ref, chunk):
    rows = from_int(in_ref[chunk, 8 * plan.slots : 8 * plan.slots + 8, :])
    down = scale_down(lower(rows))
    return down, rows * down


def pack_single(plan, ref, out_ref):
    for chunk in range(plan.chan):
        values = [plan.load(ref, chunk * plan.slots + p) for p in range(plan.slots)]
        encode_single(values, take_extra(plan, ref, chunk, 4), out_ref, chunk)


def unpack_single(plan, in_ref, ref):
    extras = []
    for chunk in range(plan.chan):
        down, extra = single_scale(plan, in_ref, chunk)
        extras.append(extra)
        for p, value in enumerate(single_tiles(plan, in_ref, chunk, down)):
            plan.store(ref, chunk * plan.slots + p, value)
    put_extra(plan, ref, extras, 4)


def store_packed(plan, first, second, out_ref):
    m = plan.main
    out_ref[:, 0:m] = first[:, 0:m].astype(bf16)
    out_ref[:, m : 2 * m] = second[:, 0:m].astype(bf16)
    if plan.tail:
        a = first[:, m : plan.wide]
        b = pltpu.roll(second[:, m : plan.wide], HALF, 1)
        out_ref[:, 2 * m :] = jnp.where(low_lanes(a.shape), a, b).astype(bf16)


def assemble(plan, pieces, blk_ref, out_ref):
    for s, piece in enumerate(pieces):
        at = pl.multiple_of((blk_ref[0] ^ s) * plan.rows, 16)
        out_ref[pl.ds(at, plan.rows), :] = piece[...]


def dot(a, b):
    return jnp.dot(a, b, preferred_element_type=f32)


def product(plan, left, right_ref, second):
    m = plan.main
    at = m if second else 0
    main = dot(left, right_ref[:, at : at + m])
    if not plan.tail:
        return main, None
    last = dot(left, right_ref[:, 2 * m :])
    return main, (pltpu.roll(last, HALF, 1) if second else last)


def commute(plan, left, right_ref, right_second, other_left, other_ref, other_second, out_ref):
    a, a_tail = product(plan, left, right_ref, right_second)
    b, b_tail = product(plan, other_left, other_ref, other_second)
    out_ref[:, 0 : plan.main] = a - b
    if plan.tail:
        out_ref[:, plan.main : plan.wide] = a_tail - b_tail


def inside_of(plan, size, blk):
    shape = (plan.rows, plan.width)
    row = lax.broadcasted_iota(jnp.int32, shape, 0) + blk[0] * plan.rows
    col = lax.broadcasted_iota(jnp.int32, shape, 1)
    return (row < size[0]) & (col < size[0])


def kernel_enter(plan, omega, ham, size, blk, send, gen_s, ham_s):
    inside = inside_of(plan, size, blk)
    gen_s[:, 0 : plan.width] = jnp.where(inside, omega[...], 0.0)
    ham_s[:, 0 : plan.width] = jnp.where(inside, ham[...], 0.0)
    pack_pair(plan, gen_s, ham_s, send)


def kernel_pair_rows(plan, omega, ham, occ, size, blk, packed, left_gen, left_ham, gen_s, ham_s):
    inside = inside_of(plan, size, blk)
    gen = jnp.where(inside, omega[...], 0.0)
    start = jnp.where(inside, ham[...], 0.0)
    gen_s[:, 0 : plan.width] = gen
    ham_s[:, 0 : plan.width] = start
    left_gen[...] = (gen * occ[...]).astype(bf16)
    left_ham[...] = (start * occ[...]).astype(bf16)
    store_packed(plan, gen_s, ham_s, packed)


def selection(plan, column_map):
    rows = lax.broadcasted_iota(jnp.int32, (plan.width, plan.width), 0)
    return (rows == column_map[...]).astype(f32).astype(bf16)


def kernel_prepare(plan, column_map, occ, moved_occ):
    w = plan.width
    hot = selection(plan, column_map)
    value = occ[...]
    high = value.astype(bf16)
    rest = value - high.astype(f32)
    middle = rest.astype(bf16)
    low = (rest - middle.astype(f32)).astype(bf16)
    total = jnp.zeros((8, w), f32)
    for part in (low, middle, high):
        total = total + lax.dot_general(
            jnp.broadcast_to(part.astype(f32), (8, w)).astype(bf16),
            hot,
            (((1,), (1,)), ((), ())),
            preferred_element_type=f32,
        )
    moved_occ[...] = total[0:1]


def kernel_unpack_cross(plan, recv, moved_occ, packed, scaled_gen, scaled_ham, gen, ham):
    unpack_pair(plan, recv, gen, ham)
    store_packed(plan, gen, ham, packed)
    scaled_gen[...] = (gen[:, 0 : plan.width] * moved_occ[...]).astype(bf16)
    scaled_ham[...] = (ham[:, 0 : plan.width] * moved_occ[...]).astype(bf16)


def keep_first(plan, right, kept):
    m = plan.main
    kept[:, 0:m] = right[:, 0:m]
    if plan.tail:
        kept[:, m:] = right[:, 2 * m :]


def kernel_cross_left(plan, scaled_gen, scaled_ham, column_map, cross_gen, cross_ham):
    select = selection(plan, column_map)
    cross_gen[...] = dot(scaled_gen[...], select).astype(bf16)
    cross_ham[...] = dot(scaled_ham[...], select).astype(bf16)


def kernel_first_pair(plan, left_gen, left_ham, blk, *refs):
    pieces, (right_gen, first, send, right) = refs[: plan.blk], refs[plan.blk :]
    assemble(plan, pieces, blk, right)
    commute(plan, left_gen[...], right, True, left_ham[...], right, False, first)
    keep_first(plan, right, right_gen)
    pack_single(plan, first, send)


def kernel_first_cross(plan, left_gen, left_ham, blk, *refs):
    pieces, (right_gen, send, right, cross_s) = refs[: plan.blk], refs[plan.blk :]
    assemble(plan, pieces, blk, right)
    commute(plan, left_gen[...], right, True, left_ham[...], right, False, cross_s)
    keep_first(plan, right, right_gen)
    pack_single(plan, cross_s, send)


def kernel_unpack_second(plan, recv, moved_occ, rows, scaled, cross):
    w = plan.width
    unpack_single(plan, recv, cross)
    rows[...] = cross[:, 0:w].astype(bf16)
    scaled[...] = (cross[:, 0:w] * moved_occ[...]).astype(bf16)


def kernel_eta_left(plan, scaled_cross, column_map, left_cross):
    left_cross[...] = dot(scaled_cross[...], selection(plan, column_map)).astype(bf16)


def kernel_second_cross(plan, left_gen, left_eta, right_gen, blk, *refs):
    pieces, (send, right, cross_s) = refs[: plan.blk], refs[plan.blk :]
    w = plan.width
    assemble(plan, pieces, blk, right)
    cross_s[:, 0:w] = dot(left_gen[...], right[...]) - dot(left_eta[...], right_gen[:, 0:w])
    pack_single(plan, cross_s, send)


def kernel_eta(plan, recv, first, occ, rows, eta, left_eta, back_s):
    w = plan.width
    unpack_single(plan, recv, back_s)
    value = back_s[:, 0:w] + first[:, 0:w]
    eta[...] = value
    rows[...] = value.astype(bf16)
    left_eta[...] = (value * occ[...]).astype(bf16)


def kernel_finish(plan, recv, ham, eta, left_gen, left_eta, right_gen, size, blk, *refs):
    pieces, (out, right, back_s) = refs[: plan.blk], refs[plan.blk :]
    w = plan.width
    assemble(plan, pieces, blk, right)
    second = dot(left_gen[...], right[...]) - dot(left_eta[...], right_gen[:, 0:w])
    unpack_single(plan, recv, back_s)
    total = ham[...] + eta[...] + 0.5 * (second + back_s[:, 0:w])
    out[...] = jnp.where(inside_of(plan, size, blk), total, 0.0)


def mixed(mixing, values, transposed):
    n = len(values)
    out = []
    for k in range(n):
        rows = [c * n + k if transposed else k * n + c for c in range(n)]
        terms = [value * mixing[pl.ds(r, value.shape[0], stride=0), :] for r, value in zip(rows, values)]
        out.append(functools.reduce(jnp.add, terms))
    return out


def kernel_mix_cross(plan, mixing, recv, send, kept):
    n = plan.chan
    scales = [pair_scale(plan, recv, c) for c in range(n)]
    extra = mixed(mixing, [s[1] for s in scales], False)
    for p in range(plan.slots):
        result = mixed(mixing, [from_int(recv[c, 16 * p : 16 * p + 16, :]) * scales[c][0] for c in range(n)], False)
        for k in range(n):
            kept[k, 16 * p : 16 * p + 16, :] = result[k]
    for k in range(n):
        values = [kept[k, 16 * p : 16 * p + 16, :] for p in range(plan.slots)]
        encode_pair(plan, values, extra[k], write_pair(send, k))


def scales_of(plan, recv):
    found = [single_scale(plan, recv, c) for c in range(plan.chan)]
    return [f[0] for f in found], [f[1] for f in found]


def groups_of(plan):
    return [(p, min(2, plan.slots - p)) for p in range(0, plan.slots, 2)]


def tiles_of(plan, recv, scales, p, n):
    wide = [jnp.concatenate([x] * n, axis=0) for x in scales]
    return [from_int(recv[c, 8 * p : 8 * (p + n), :]) * wide[c] for c in range(plan.chan)]


def encode_all(plan, kept, extra, send):
    for k in range(plan.chan):
        values = [kept[k, 8 * p : 8 * p + 8, :] for p in range(plan.slots)]
        encode_single(values, extra[k], send, k)


def kernel_mix_back(plan, mixing, recv, send, kept):
    scales, extra = scales_of(plan, recv)
    for p, n in groups_of(plan):
        for k, value in enumerate(mixed(mixing, tiles_of(plan, recv, scales, p, n), True)):
            kept[k, 8 * p : 8 * (p + n), :] = value
    encode_all(plan, kept, mixed(mixing, extra, True), send)


def kernel_mix_both(plan, mixing, recv, recv_first, send, send_back, kept, kept_back):
    scales, extra = scales_of(plan, recv)
    scales_first, extra_first = scales_of(plan, recv_first)

    def both(value, first):
        back = mixed(mixing, value, True)
        return back, mixed(mixing, [f + r for f, r in zip(first, back)], False)

    for p, n in groups_of(plan):
        back, cross = both(tiles_of(plan, recv, scales, p, n), tiles_of(plan, recv_first, scales_first, p, n))
        for k in range(plan.chan):
            kept_back[k, 8 * p : 8 * (p + n), :] = back[k]
            kept[k, 8 * p : 8 * (p + n), :] = cross[k]
    extra_back, extra = both(extra, extra_first)
    encode_all(plan, kept, extra, send)
    encode_all(plan, kept_back, extra_back, send_back)


def plain_mix(plan, kind, mixing, recv, recv_first=None):
    n, slots = plan.chan, plan.slots
    high = 16 if kind == "cross" else 8

    def mix(spec, value):
        return jnp.einsum(spec, mixing, value, precision=exact_mode, preferred_element_type=f32)

    def spread_rows(e):
        if kind == "cross":
            return jnp.concatenate([e[:, 0:4]] * 2 + [e[:, 4:8]] * 2, axis=1)
        return jnp.concatenate([e[:, 0:4]] * 2, axis=1)

    def decode(chunks):
        raw = chunks.astype(jnp.int32).astype(f32)
        e = raw[:, high * slots : high * slots + 8]
        return raw[:, 0 : high * slots].reshape(n, slots, high, 128) * scale_down(spread_rows(e))[:, None]

    def encode(value):
        peak = jnp.max(jnp.abs(value), axis=1)
        peak = jnp.max(peak.reshape(n, high // 8, 2, 4, 128), axis=2).reshape(n, high // 2, 128)
        e = exponent_of(peak)
        scaled = value * scale_up(spread_rows(e))[:, None]
        out = jnp.concatenate([scaled.reshape(n, -1, 128), e], axis=1)
        return to_int(jnp.pad(out, ((0, 0), (0, recv.shape[1] - out.shape[1]), (0, 0))))

    if kind == "cross":
        return encode(mix("kc,cpsl->kpsl", decode(recv)))
    back = mix("ck,cpsl->kpsl", decode(recv))
    if kind == "back":
        return encode(back)
    return encode(mix("kc,cpsl->kpsl", decode(recv_first) + back)), encode(back)


def call(body, plan, outs, specs, scratch=(), flops=0, final=False):
    def run(*operands):
        places = {"v": pltpu.VMEM, "h": pltpu.HBM}
        placed = [
            pltpu.with_memory_space_constraint(x, places[s]) if s in places else x
            for x, s in zip(operands, specs, strict=True)
        ]
        return pl.pallas_call(
            functools.partial(body, plan),
            out_shape=tuple((jax.ShapeDtypeStruct if final else pltpu.VMEM)(s, d) for s, d in outs),
            in_specs=[smem() if s == "s" else vmem() for s in specs],
            out_specs=tuple(vmem() for _ in outs),
            scratch_shapes=tuple(pltpu.VMEM(s, d) for s, d in scratch),
            cost_estimate=pl.CostEstimate(flops=flops or plan.rows * plan.width * 60000, transcendentals=0, bytes_accessed=0),
            compiler_params=pltpu.CompilerParams(vmem_limit_bytes=GRANT),
        )(*placed)

    return run


MIXERS = {"cross": kernel_mix_cross, "both": kernel_mix_both, "back": kernel_mix_back}


def mix_call(plan, kind, mixing, *recv):
    if plan.chan > UNROLLED:
        return plain_mix(plan, kind, mixing, *recv)
    rows = recv[0].shape[1]
    outs = call(
        MIXERS[kind],
        plan,
        [((plan.chan, rows, 128), i16)] * len(recv),
        "v" * (1 + len(recv)),
        [((plan.chan, rows, 128), f32)] * len(recv),
    )(mixing, *recv)
    return outs if len(recv) > 1 else outs[0]


def mixing_matrix(jlabel, family, sixj):
    levels = sixj.shape[0]
    one_hot = (jlabel[:, None] == jnp.arange(levels, dtype=jnp.int32)[None, :]).astype(f32)
    picked = jnp.dot(one_hot, sixj, precision=exact_mode, preferred_element_type=f32)
    picked = jnp.dot(picked, one_hot.T, precision=exact_mode, preferred_element_type=f32)
    kindred = (family[:, None] == family[None, :]).astype(f32)
    return picked * kindred


def swap(value, size, bits):
    return lax.ppermute(value, "blk", [(b, b ^ bits) for b in range(size)])


def far_rows(value, size):
    return swap(value, size, size // 2) if size > 1 else None


def near_rows(value, far, size):
    pieces = {0: value}
    bit = size // 2
    while bit:
        for s, piece in list(pieces.items()):
            pieces[s ^ bit] = far if bit == size // 2 and s == 0 else swap(piece, size, bit)
        bit //= 2
    return [pieces[s] for s in range(size)]


def exchange(value):
    return lax.all_to_all(value, "chan", 0, 0, tiled=True)


def on_device(omega, hamiltonian, pair_occ, cross_occ, block_size, jlabel, family, sixj, column_map):
    channels_here, rows, width = omega.shape
    assert channels_here == 1
    chan, blk = lax.axis_size("chan"), lax.axis_size("blk")
    assert blk & (blk - 1) == 0
    plan = Plan(rows, width, chan, blk)
    omega, ham = omega[0], hamiltonian[0]
    blk_index = lax.axis_index("blk").astype(jnp.int32).reshape(1)
    pair = ((chan, plan.pair_rows, 128), i16)
    single = ((chan, plan.single_rows, 128), i16)
    packed = ((rows, plan.packed), bf16)
    left = ((rows, width), bf16)
    plain = ((rows, width), f32)
    wide = ((rows, plan.wide), f32)
    right = ((rows * blk, plan.packed), bf16)
    right_kept = ((rows * blk, plan.wide), bf16)
    right_one = ((rows * blk, width), bf16)

    (send,) = call(kernel_enter, plan, [pair], "hhss", [wide, wide])(omega, ham, block_size, blk_index)
    pair_rows, left_gen, left_ham = call(kernel_pair_rows, plan, [packed, left, left], "hhhss", [wide, wide])(
        omega, ham, pair_occ, block_size, blk_index
    )
    column_row = column_map.reshape(1, width)
    (moved_occ,) = call(kernel_prepare, plan, [((1, width), f32)], "vv")(column_row, cross_occ)
    mixing = mixing_matrix(jlabel, family, sixj)
    if chan <= UNROLLED:
        mixing = jnp.broadcast_to(mixing.reshape(chan * chan, 1), (chan * chan, 128))
    pair_far = far_rows(pair_rows, blk)
    recv = exchange(send)
    recv, mixing, moved_occ = lax.optimization_barrier((recv, mixing, moved_occ))

    pair_pieces = near_rows(pair_rows, pair_far, blk)
    recv = exchange(mix_call(plan, "cross", mixing, recv))
    pair_right, first, send_first = call(
        kernel_first_pair, plan, [right_kept, wide, single], "vvs" + "v" * blk, [right]
    )(left_gen, left_ham, blk_index, *pair_pieces)
    recv, pair_right, first, send_first = lax.optimization_barrier((recv, pair_right, first, send_first))
    cross_rows, scaled_gen, scaled_ham = call(
        kernel_unpack_cross, plan, [packed, left, left], "vv", [wide, wide]
    )(recv, moved_occ)
    cross_rows, send_first = lax.optimization_barrier((cross_rows, send_first))
    cross_far = far_rows(cross_rows, blk)
    recv_first = exchange(send_first)
    cross_gen_left, cross_ham_left = call(kernel_cross_left, plan, [left, left], "vvv")(
        scaled_gen, scaled_ham, column_row
    )
    cross_far, cross_gen_left, cross_ham_left = lax.optimization_barrier((cross_far, cross_gen_left, cross_ham_left))
    cross_pieces = near_rows(cross_rows, cross_far, blk)
    cross_right, send = call(
        kernel_first_cross, plan, [right_kept, single], "vvs" + "v" * blk, [right, wide]
    )(cross_gen_left, cross_ham_left, blk_index, *cross_pieces)
    send, recv_first = lax.optimization_barrier((send, recv_first))

    send, send_back = mix_call(plan, "both", mixing, exchange(send), recv_first)
    recv = exchange(send)
    recv, send_back = lax.optimization_barrier((recv, send_back))
    second_rows, scaled = call(kernel_unpack_second, plan, [left, left], "vv", [wide])(recv, moved_occ)
    second_far = far_rows(second_rows, blk)
    recv_back = exchange(send_back)
    (cross_eta_left,) = call(kernel_eta_left, plan, [left], "vv")(scaled, column_row)
    second_far, cross_eta_left = lax.optimization_barrier((second_far, cross_eta_left))
    second_pieces = near_rows(second_rows, second_far, blk)
    (send,) = call(kernel_second_cross, plan, [single], "vvvs" + "v" * blk, [right_one, wide])(
        cross_gen_left, cross_eta_left, cross_right, blk_index, *second_pieces
    )
    send, recv_back = lax.optimization_barrier((send, recv_back))

    recv = exchange(send)
    eta_rows, eta, left_eta = call(kernel_eta, plan, [left, plain, left], "vvv", [wide])(recv_back, first, pair_occ)
    eta_far = far_rows(eta_rows, blk)
    eta_pieces = near_rows(eta_rows, eta_far, blk)
    recv, eta_pieces = lax.optimization_barrier((recv, eta_pieces))
    recv = exchange(mix_call(plan, "back", mixing, recv))
    (out,) = call(kernel_finish, plan, [plain], "vvvvvvss" + "v" * blk, [right_one, wide], final=True)(
        recv, ham, eta, left_gen, left_eta, pair_right, block_size, blk_index, *eta_pieces
    )
    return out[None]


def solution(mesh):
    in_specs = (
        P("chan", "blk", None),
        P("chan", "blk", None),
        P("chan", None),
        P("chan", None),
        P("chan"),
        P(),
        P(),
        P(),
        P(),
    )
    out_specs = P("chan", "blk", None)
    return jax.shard_map(on_device, mesh=mesh, in_specs=in_specs, out_specs=out_specs, check_vma=False)
```

```python
import functools

import jax
import jax.numpy as jnp
from jax import lax
from jax.experimental import pallas as pl
from jax.experimental.pallas import tpu as pltpu
from jax.sharding import PartitionSpec as P

exact_mode = lax.Precision.HIGHEST
f32 = jnp.float32
bf16 = jnp.bfloat16
i16 = jnp.int16
LEVELS = 32760.0
STEP = 0.08664339756999316
TINY = 1e-30
HALF = 64
UNROLLED = 16
GRANT = 12 << 20


def vmem():
    return pl.BlockSpec(memory_space=pltpu.VMEM)


def smem():
    return pl.BlockSpec(memory_space=pltpu.SMEM)


class Plan:
    def __init__(self, rows, width, chan, blk):
        assert rows % 16 == 0 and width % 128 in (0, HALF) and width >= 128
        self.rows, self.width, self.chan, self.blk = rows, width, chan, blk
        self.full = width // 128
        self.tail = width % 128 != 0
        self.groups = rows // 8
        self.main = self.full * 128
        self.wide = self.main + (128 if self.tail else 0)
        self.packed = 2 * self.main + (128 if self.tail else 0)
        self.tiles = self.groups * self.full + (self.groups // 2 if self.tail else 0)
        self.slots, rest = divmod(self.tiles, chan)
        self.extra = 0
        if rest and chan <= UNROLLED and 8 * rest % chan == 0 and 8 * rest // chan <= 4 and self.slots:
            self.extra = 8 * rest // chan
        elif rest:
            self.slots += 1
        self.pair_rows = 16 * (self.slots + 1)
        self.single_rows = 8 * (self.slots + 1)

    def load(self, ref, u):
        if u >= self.tiles:
            return jnp.zeros((8, 128), f32)
        if u < self.groups * self.full:
            g, j = divmod(u, self.full)
            return ref[8 * g : 8 * g + 8, 128 * j : 128 * j + 128]
        v = 16 * (u - self.groups * self.full)
        first = ref[v : v + 8, self.main : self.wide]
        second = pltpu.roll(ref[v + 8 : v + 16, self.main : self.wide], HALF, 1)
        return jnp.where(low_lanes((8, 128)), first, second)

    def store(self, ref, u, tile):
        if u >= self.tiles:
            return
        if u < self.groups * self.full:
            g, j = divmod(u, self.full)
            ref[8 * g : 8 * g + 8, 128 * j : 128 * j + 128] = tile
            return
        v = 16 * (u - self.groups * self.full)
        ref[v : v + 8, self.main : self.wide] = tile
        ref[v + 8 : v + 16, self.main : self.wide] = pltpu.roll(tile, HALF, 1)


def low_lanes(shape):
    return lax.broadcasted_iota(jnp.int32, shape, len(shape) - 1) < HALF


def sublane():
    return lax.broadcasted_iota(jnp.int32, (8, 128), 0)


def turn(tile, by):
    by %= 8
    return pltpu.roll(tile, by, 0) if by else tile


def lower(tile):
    return jnp.where(sublane() < 4, tile, turn(tile, 4))


def spread(tile):
    other = turn(tile, 4)
    low = sublane() < 4
    return jnp.concatenate([jnp.where(low, tile, other), jnp.where(low, other, tile)], axis=0)


def exponent_of(peak):
    return jnp.floor(jnp.log(jnp.maximum(peak, TINY)) * (1.0 / STEP)) + 1.0


def scale_up(e):
    return jnp.exp(e * -STEP) * LEVELS


def scale_down(e):
    return jnp.exp(e * STEP) * (1.0 / LEVELS)


def to_int(value):
    return jnp.round(value).astype(jnp.int32).astype(i16)


def from_int(value):
    return value.astype(jnp.int32).astype(f32)


def largest(values):
    return functools.reduce(jnp.maximum, [jnp.abs(v) for v in values])


def take_extra(plan, ref, chunk, at):
    out = jnp.zeros((8, 128), f32)
    for m in range(plan.extra):
        tile, row = divmod(chunk * plan.extra + m, 8)
        value = plan.load(ref, plan.chan * plan.slots + tile)
        out = jnp.where(sublane() == at + m, turn(value, at + m - row), out)
    return out


def put_extra(plan, ref, extras, at):
    if not plan.extra:
        return
    tiles = [jnp.zeros((8, 128), f32) for _ in range(plan.chan * plan.extra // 8)]
    for chunk, value in enumerate(extras):
        for m in range(plan.extra):
            tile, row = divmod(chunk * plan.extra + m, 8)
            tiles[tile] = jnp.where(sublane() == row, turn(value, row - at - m), tiles[tile])
    for tile, value in enumerate(tiles):
        plan.store(ref, plan.chan * plan.slots + tile, value)


def encode_pair(plan, values, extra, write):
    peak = largest(values)
    first = jnp.maximum(peak[0:8], turn(peak[0:8], 4))
    second = jnp.maximum(peak[8:16], turn(peak[8:16], 4))
    peak = jnp.maximum(jnp.where(sublane() < 4, first, second), jnp.abs(extra))
    e = exponent_of(peak)
    up = scale_up(e)
    both = spread(up)
    for p, v in enumerate(values):
        write(p, to_int(v * both))
    write(plan.slots, to_int(jnp.concatenate([e, extra * up], axis=0)))


def pair_scale(plan, in_ref, chunk):
    last = from_int(in_ref[chunk, 16 * plan.slots : 16 * plan.slots + 16, :])
    down = scale_down(last[0:8])
    return spread(down), last[8:16] * down


def write_pair(out_ref, chunk):
    def write(p, tile):
        out_ref[chunk, 16 * p : 16 * p + 16, :] = tile

    return write


def pack_pair(plan, first_ref, second_ref, out_ref):
    for chunk in range(plan.chan):
        us = [chunk * plan.slots + p for p in range(plan.slots)]
        values = [jnp.concatenate([plan.load(first_ref, u), plan.load(second_ref, u)], axis=0) for u in us]
        extra = take_extra(plan, first_ref, chunk, 0) + take_extra(plan, second_ref, chunk, 4)
        encode_pair(plan, values, extra, write_pair(out_ref, chunk))


def unpack_pair(plan, in_ref, first_ref, second_ref):
    extras = []
    for chunk in range(plan.chan):
        down, extra = pair_scale(plan, in_ref, chunk)
        extras.append(extra)
        for p in range(plan.slots):
            u = chunk * plan.slots + p
            if u < plan.tiles:
                v = from_int(in_ref[chunk, 16 * p : 16 * p + 16, :]) * down
                plan.store(first_ref, u, v[0:8])
                plan.store(second_ref, u, v[8:16])
    put_extra(plan, first_ref, extras, 0)
    put_extra(plan, second_ref, extras, 4)


def encode_single(values, extra, out_ref, chunk):
    peak = jnp.maximum(largest(values), jnp.abs(extra))
    e = exponent_of(jnp.maximum(peak, turn(peak, 4)))
    up = scale_up(e)
    scaled = [v * up for v in values] + [jnp.where(sublane() < 4, e, extra * up)]
    for p in range(0, len(scaled), 2):
        part = scaled[p : p + 2]
        out_ref[chunk, 8 * p : 8 * (p + len(part)), :] = to_int(jnp.concatenate(part, axis=0))


def single_tiles(plan, in_ref, chunk, scale):
    values = []
    for p in range(0, plan.slots, 2):
        n = min(2, plan.slots - p)
        rows = from_int(in_ref[chunk, 8 * p : 8 * (p + n), :])
        values += [rows[8 * q : 8 * q + 8] * scale for q in range(n)]
    return values


def single_scale(plan, in_ref, chunk):
    rows = from_int(in_ref[chunk, 8 * plan.slots : 8 * plan.slots + 8, :])
    down = scale_down(lower(rows))
    return down, rows * down


def pack_single(plan, ref, out_ref):
    for chunk in range(plan.chan):
        values = [plan.load(ref, chunk * plan.slots + p) for p in range(plan.slots)]
        encode_single(values, take_extra(plan, ref, chunk, 4), out_ref, chunk)


def unpack_single(plan, in_ref, ref):
    extras = []
    for chunk in range(plan.chan):
        down, extra = single_scale(plan, in_ref, chunk)
        extras.append(extra)
        for p, value in enumerate(single_tiles(plan, in_ref, chunk, down)):
            plan.store(ref, chunk * plan.slots + p, value)
    put_extra(plan, ref, extras, 4)


def store_packed(plan, first, second, out_ref):
    m = plan.main
    out_ref[:, 0:m] = first[:, 0:m].astype(bf16)
    out_ref[:, m : 2 * m] = second[:, 0:m].astype(bf16)
    if plan.tail:
        a = first[:, m : plan.wide]
        b = pltpu.roll(second[:, m : plan.wide], HALF, 1)
        out_ref[:, 2 * m :] = jnp.where(low_lanes(a.shape), a, b).astype(bf16)


def assemble(plan, pieces, blk_ref, out_ref):
    for s, piece in enumerate(pieces):
        at = pl.multiple_of((blk_ref[0] ^ s) * plan.rows, 16)
        out_ref[pl.ds(at, plan.rows), :] = piece[...]


def dot(a, b):
    return jnp.dot(a, b, preferred_element_type=f32)


def product(plan, left, right_ref, second):
    m = plan.main
    at = m if second else 0
    main = dot(left, right_ref[:, at : at + m])
    if not plan.tail:
        return main, None
    last = dot(left, right_ref[:, 2 * m :])
    return main, (pltpu.roll(last, HALF, 1) if second else last)


def commute(plan, left, right_ref, right_second, other_left, other_ref, other_second, out_ref):
    a, a_tail = product(plan, left, right_ref, right_second)
    b, b_tail = product(plan, other_left, other_ref, other_second)
    out_ref[:, 0 : plan.main] = a - b
    if plan.tail:
        out_ref[:, plan.main : plan.wide] = a_tail - b_tail


def inside_of(plan, size, blk):
    shape = (plan.rows, plan.width)
    row = lax.broadcasted_iota(jnp.int32, shape, 0) + blk[0] * plan.rows
    col = lax.broadcasted_iota(jnp.int32, shape, 1)
    return (row < size[0]) & (col < size[0])


def kernel_enter(plan, omega, ham, size, blk, send, gen_s, ham_s):
    inside = inside_of(plan, size, blk)
    gen_s[:, 0 : plan.width] = jnp.where(inside, omega[...], 0.0)
    ham_s[:, 0 : plan.width] = jnp.where(inside, ham[...], 0.0)
    pack_pair(plan, gen_s, ham_s, send)


def kernel_pair_rows(plan, omega, ham, occ, size, blk, packed, left_gen, left_ham, gen_s, ham_s):
    inside = inside_of(plan, size, blk)
    gen = jnp.where(inside, omega[...], 0.0)
    start = jnp.where(inside, ham[...], 0.0)
    gen_s[:, 0 : plan.width] = gen
    ham_s[:, 0 : plan.width] = start
    left_gen[...] = (gen * occ[...]).astype(bf16)
    left_ham[...] = (start * occ[...]).astype(bf16)
    store_packed(plan, gen_s, ham_s, packed)


def selection(plan, column_map):
    rows = lax.broadcasted_iota(jnp.int32, (plan.width, plan.width), 0)
    return (rows == column_map[...]).astype(f32).astype(bf16)


def kernel_prepare(plan, column_map, occ, moved_occ):
    w = plan.width
    hot = selection(plan, column_map)
    value = occ[...]
    high = value.astype(bf16)
    rest = value - high.astype(f32)
    middle = rest.astype(bf16)
    low = (rest - middle.astype(f32)).astype(bf16)
    total = jnp.zeros((8, w), f32)
    for part in (low, middle, high):
        total = total + lax.dot_general(
            jnp.broadcast_to(part.astype(f32), (8, w)).astype(bf16),
            hot,
            (((1,), (1,)), ((), ())),
            preferred_element_type=f32,
        )
    moved_occ[...] = total[0:1]


def kernel_unpack_cross(plan, recv, moved_occ, packed, scaled_gen, scaled_ham, gen, ham):
    unpack_pair(plan, recv, gen, ham)
    store_packed(plan, gen, ham, packed)
    scaled_gen[...] = (gen[:, 0 : plan.width] * moved_occ[...]).astype(bf16)
    scaled_ham[...] = (ham[:, 0 : plan.width] * moved_occ[...]).astype(bf16)


def keep_first(plan, right, kept):
    m = plan.main
    kept[:, 0:m] = right[:, 0:m]
    if plan.tail:
        kept[:, m:] = right[:, 2 * m :]


def kernel_cross_left(plan, scaled_gen, scaled_ham, column_map, cross_gen, cross_ham):
    select = selection(plan, column_map)
    cross_gen[...] = dot(scaled_gen[...], select).astype(bf16)
    cross_ham[...] = dot(scaled_ham[...], select).astype(bf16)


def kernel_first_pair(plan, left_gen, left_ham, blk, *refs):
    pieces, (right_gen, first, send, right) = refs[: plan.blk], refs[plan.blk :]
    assemble(plan, pieces, blk, right)
    commute(plan, left_gen[...], right, True, left_ham[...], right, False, first)
    keep_first(plan, right, right_gen)
    pack_single(plan, first, send)


def kernel_first_cross(plan, left_gen, left_ham, blk, *refs):
    pieces, (right_gen, send, right, cross_s) = refs[: plan.blk], refs[plan.blk :]
    assemble(plan, pieces, blk, right)
    commute(plan, left_gen[...], right, True, left_ham[...], right, False, cross_s)
    keep_first(plan, right, right_gen)
    pack_single(plan, cross_s, send)


def kernel_unpack_second(plan, recv, first, moved_occ, rows, scaled, eta, eta_rows, eta_s, cross):
    w = plan.width
    unpack_pair(plan, recv, eta_s, cross)
    rows[...] = cross[:, 0:w].astype(bf16)
    scaled[...] = (cross[:, 0:w] * moved_occ[...]).astype(bf16)
    value = eta_s[:, 0:w] + first[:, 0:w]
    eta[...] = value
    eta_rows[...] = value.astype(bf16)


def kernel_eta_left(plan, scaled_cross, column_map, left_cross):
    left_cross[...] = dot(scaled_cross[...], selection(plan, column_map)).astype(bf16)


def kernel_second_cross(plan, left_gen, left_eta, right_gen, blk, *refs):
    pieces, (send, right, cross_s) = refs[: plan.blk], refs[plan.blk :]
    w = plan.width
    assemble(plan, pieces, blk, right)
    cross_s[:, 0:w] = dot(left_gen[...], right[...]) - dot(left_eta[...], right_gen[:, 0:w])
    pack_single(plan, cross_s, send)


def kernel_eta_right(plan, blk, *refs):
    assemble(plan, refs[: plan.blk], blk, refs[plan.blk])


def kernel_finish(plan, recv, ham, eta, left_gen, occ, right, right_gen, size, blk, out, back_s):
    w = plan.width
    left_eta = (eta[...] * occ[...]).astype(bf16)
    second = dot(left_gen[...], right[...]) - dot(left_eta, right_gen[:, 0:w])
    unpack_single(plan, recv, back_s)
    total = ham[...] + eta[...] + 0.5 * (second + back_s[:, 0:w])
    out[...] = jnp.where(inside_of(plan, size, blk), total, 0.0)


def mixed(mixing, values, transposed):
    n = len(values)
    out = []
    for k in range(n):
        rows = [c * n + k if transposed else k * n + c for c in range(n)]
        terms = [value * mixing[pl.ds(r, value.shape[0], stride=0), :] for r, value in zip(rows, values)]
        out.append(functools.reduce(jnp.add, terms))
    return out


def kernel_mix_cross(plan, mixing, recv, send, kept):
    n = plan.chan
    scales = [pair_scale(plan, recv, c) for c in range(n)]
    extra = mixed(mixing, [s[1] for s in scales], False)
    for p in range(plan.slots):
        result = mixed(mixing, [from_int(recv[c, 16 * p : 16 * p + 16, :]) * scales[c][0] for c in range(n)], False)
        for k in range(n):
            kept[k, 16 * p : 16 * p + 16, :] = result[k]
    for k in range(n):
        values = [kept[k, 16 * p : 16 * p + 16, :] for p in range(plan.slots)]
        encode_pair(plan, values, extra[k], write_pair(send, k))


def scales_of(plan, recv):
    found = [single_scale(plan, recv, c) for c in range(plan.chan)]
    return [f[0] for f in found], [f[1] for f in found]


def groups_of(plan):
    return [(p, min(2, plan.slots - p)) for p in range(0, plan.slots, 2)]


def tiles_of(plan, recv, scales, p, n):
    wide = [jnp.concatenate([x] * n, axis=0) for x in scales]
    return [from_int(recv[c, 8 * p : 8 * (p + n), :]) * wide[c] for c in range(plan.chan)]


def encode_all(plan, kept, extra, send):
    for k in range(plan.chan):
        values = [kept[k, 8 * p : 8 * p + 8, :] for p in range(plan.slots)]
        encode_single(values, extra[k], send, k)


def kernel_mix_back(plan, mixing, recv, send, kept):
    scales, extra = scales_of(plan, recv)
    for p, n in groups_of(plan):
        for k, value in enumerate(mixed(mixing, tiles_of(plan, recv, scales, p, n), True)):
            kept[k, 8 * p : 8 * (p + n), :] = value
    encode_all(plan, kept, mixed(mixing, extra, True), send)


def kernel_mix_both(plan, mixing, recv, recv_first, send, kept):
    scales, extra = scales_of(plan, recv)
    scales_first, extra_first = scales_of(plan, recv_first)

    def both(value, first):
        back = mixed(mixing, value, True)
        return back, mixed(mixing, [f + r for f, r in zip(first, back)], False)

    for p, n in groups_of(plan):
        back, cross = both(tiles_of(plan, recv, scales, p, n), tiles_of(plan, recv_first, scales_first, p, n))
        for k in range(plan.chan):
            for q in range(n):
                at, rows = 16 * (p + q), slice(8 * q, 8 * q + 8)
                kept[k, at : at + 8, :] = back[k][rows]
                kept[k, at + 8 : at + 16, :] = cross[k][rows]
    extra_back, extra_cross = both(extra, extra_first)
    for k in range(plan.chan):
        values = [kept[k, 16 * p : 16 * p + 16, :] for p in range(plan.slots)]
        extra = jnp.where(sublane() < 4, turn(extra_back[k], 4), extra_cross[k])
        encode_pair(plan, values, extra, write_pair(send, k))


def plain_mix(plan, kind, mixing, recv, recv_first=None):
    n, slots = plan.chan, plan.slots

    def mix(spec, value):
        return jnp.einsum(spec, mixing, value, precision=exact_mode, preferred_element_type=f32)

    def spread_rows(e, high):
        return jnp.concatenate([e[:, 0:4]] * 2 + ([e[:, 4:8]] * 2 if high == 16 else []), axis=1)

    def decode(chunks, high):
        raw = chunks.astype(jnp.int32).astype(f32)
        e = raw[:, high * slots : high * slots + 8]
        return raw[:, 0 : high * slots].reshape(n, slots, high, 128) * scale_down(spread_rows(e, high))[:, None]

    def encode(value, high, rows):
        peak = jnp.max(jnp.abs(value), axis=1)
        peak = jnp.max(peak.reshape(n, high // 8, 2, 4, 128), axis=2).reshape(n, high // 2, 128)
        e = exponent_of(peak)
        scaled = value * scale_up(spread_rows(e, high))[:, None]
        out = jnp.concatenate([scaled.reshape(n, -1, 128), e], axis=1)
        return to_int(jnp.pad(out, ((0, 0), (0, rows - out.shape[1]), (0, 0))))

    if kind == "cross":
        return encode(mix("kc,cpsl->kpsl", decode(recv, 16)), 16, plan.pair_rows)
    back = mix("ck,cpsl->kpsl", decode(recv, 8))
    if kind == "back":
        return encode(back, 8, plan.single_rows)
    cross = mix("kc,cpsl->kpsl", decode(recv_first, 8) + back)
    return encode(jnp.concatenate([back, cross], axis=2), 16, plan.pair_rows)


def call(body, plan, outs, specs, scratch=(), flops=0, final=False):
    def run(*operands):
        places = {"v": pltpu.VMEM, "h": pltpu.HBM}
        placed = [
            pltpu.with_memory_space_constraint(x, places[s]) if s in places else x
            for x, s in zip(operands, specs, strict=True)
        ]
        return pl.pallas_call(
            functools.partial(body, plan),
            out_shape=tuple((jax.ShapeDtypeStruct if final else pltpu.VMEM)(s, d) for s, d in outs),
            in_specs=[smem() if s == "s" else vmem() for s in specs],
            out_specs=tuple(vmem() for _ in outs),
            scratch_shapes=tuple(pltpu.VMEM(s, d) for s, d in scratch),
            cost_estimate=pl.CostEstimate(flops=flops or plan.rows * plan.width * 60000, transcendentals=0, bytes_accessed=0),
            compiler_params=pltpu.CompilerParams(vmem_limit_bytes=GRANT),
        )(*placed)

    return run


MIXERS = {"cross": kernel_mix_cross, "both": kernel_mix_both, "back": kernel_mix_back}


def mix_call(plan, kind, mixing, *recv):
    if plan.chan > UNROLLED:
        return plain_mix(plan, kind, mixing, *recv)
    rows = plan.single_rows if kind == "back" else plan.pair_rows
    shape = (plan.chan, rows, 128)
    (made,) = call(MIXERS[kind], plan, [(shape, i16)], "v" * (1 + len(recv)), [(shape, f32)])(mixing, *recv)
    return made


def mixing_matrix(jlabel, family, sixj):
    levels = sixj.shape[0]
    one_hot = (jlabel[:, None] == jnp.arange(levels, dtype=jnp.int32)[None, :]).astype(f32)
    picked = jnp.dot(one_hot, sixj, precision=exact_mode, preferred_element_type=f32)
    picked = jnp.dot(picked, one_hot.T, precision=exact_mode, preferred_element_type=f32)
    kindred = (family[:, None] == family[None, :]).astype(f32)
    return picked * kindred


def swap(value, size, bits):
    return lax.ppermute(value, "blk", [(b, b ^ bits) for b in range(size)])


def far_rows(value, size):
    return swap(value, size, size // 2) if size > 1 else None


def near_rows(value, far, size):
    pieces = {0: value}
    bit = size // 2
    while bit:
        for s, piece in list(pieces.items()):
            pieces[s ^ bit] = far if bit == size // 2 and s == 0 else swap(piece, size, bit)
        bit //= 2
    return [pieces[s] for s in range(size)]


def exchange(value):
    return lax.all_to_all(value, "chan", 0, 0, tiled=True)


def on_device(omega, hamiltonian, pair_occ, cross_occ, block_size, jlabel, family, sixj, column_map):
    channels_here, rows, width = omega.shape
    assert channels_here == 1
    chan, blk = lax.axis_size("chan"), lax.axis_size("blk")
    assert blk & (blk - 1) == 0
    plan = Plan(rows, width, chan, blk)
    omega, ham = omega[0], hamiltonian[0]
    blk_index = lax.axis_index("blk").astype(jnp.int32).reshape(1)
    pair = ((chan, plan.pair_rows, 128), i16)
    single = ((chan, plan.single_rows, 128), i16)
    packed = ((rows, plan.packed), bf16)
    left = ((rows, width), bf16)
    plain = ((rows, width), f32)
    wide = ((rows, plan.wide), f32)
    right = ((rows * blk, plan.packed), bf16)
    right_kept = ((rows * blk, plan.wide), bf16)
    right_one = ((rows * blk, width), bf16)

    (send,) = call(kernel_enter, plan, [pair], "hhss", [wide, wide])(omega, ham, block_size, blk_index)
    pair_rows, left_gen, left_ham = call(kernel_pair_rows, plan, [packed, left, left], "hhhss", [wide, wide])(
        omega, ham, pair_occ, block_size, blk_index
    )
    column_row = column_map.reshape(1, width)
    (moved_occ,) = call(kernel_prepare, plan, [((1, width), f32)], "vv")(column_row, cross_occ)
    mixing = mixing_matrix(jlabel, family, sixj)
    if chan <= UNROLLED:
        mixing = jnp.broadcast_to(mixing.reshape(chan * chan, 1), (chan * chan, 128))
    pair_far = far_rows(pair_rows, blk)
    recv = exchange(send)
    recv, mixing, moved_occ = lax.optimization_barrier((recv, mixing, moved_occ))

    pair_pieces = near_rows(pair_rows, pair_far, blk)
    recv = exchange(mix_call(plan, "cross", mixing, recv))
    pair_right, first, send_first = call(
        kernel_first_pair, plan, [right_kept, wide, single], "vvs" + "v" * blk, [right]
    )(left_gen, left_ham, blk_index, *pair_pieces)
    recv, pair_right, first, send_first = lax.optimization_barrier((recv, pair_right, first, send_first))
    cross_rows, scaled_gen, scaled_ham = call(
        kernel_unpack_cross, plan, [packed, left, left], "vv", [wide, wide]
    )(recv, moved_occ)
    cross_rows, send_first = lax.optimization_barrier((cross_rows, send_first))
    cross_far = far_rows(cross_rows, blk)
    recv_first = exchange(send_first)
    cross_gen_left, cross_ham_left = call(kernel_cross_left, plan, [left, left], "vvv")(
        scaled_gen, scaled_ham, column_row
    )
    cross_far, cross_gen_left, cross_ham_left = lax.optimization_barrier((cross_far, cross_gen_left, cross_ham_left))
    cross_pieces = near_rows(cross_rows, cross_far, blk)
    cross_right, send = call(
        kernel_first_cross, plan, [right_kept, single], "vvs" + "v" * blk, [right, wide]
    )(cross_gen_left, cross_ham_left, blk_index, *cross_pieces)
    send, recv_first = lax.optimization_barrier((send, recv_first))

    recv = exchange(mix_call(plan, "both", mixing, exchange(send), recv_first))
    second_rows, scaled, eta, eta_rows = call(
        kernel_unpack_second, plan, [left, left, plain, left], "vvv", [wide, wide]
    )(recv, first, moved_occ)
    second_far = far_rows(second_rows, blk)
    (cross_eta_left,) = call(kernel_eta_left, plan, [left], "vv")(scaled, column_row)
    second_far, cross_eta_left = lax.optimization_barrier((second_far, cross_eta_left))
    second_pieces = near_rows(second_rows, second_far, blk)
    (send,) = call(kernel_second_cross, plan, [single], "vvvs" + "v" * blk, [right_one, wide])(
        cross_gen_left, cross_eta_left, cross_right, blk_index, *second_pieces
    )
    recv = exchange(send)
    eta_pieces = [eta_rows] + [swap(eta_rows, blk, s) for s in range(1, blk // 2)]
    eta_pieces += [swap(eta_rows, blk, blk // 2)]
    eta_pieces += [swap(eta_rows, blk, s) for s in range(blk // 2 + 1, blk)]
    send = mix_call(plan, "back", mixing, recv)
    (eta_right,) = call(kernel_eta_right, plan, [right_one], "s" + "v" * blk)(blk_index, *eta_pieces)
    send, eta_right = lax.optimization_barrier((send, eta_right))
    recv = exchange(send)
    (out,) = call(kernel_finish, plan, [plain], "vvvvvvvss", [wide], final=True)(
        recv, ham, eta, left_gen, pair_occ, eta_right, pair_right, block_size, blk_index
    )
    return out[None]


def solution(mesh):
    in_specs = (
        P("chan", "blk", None),
        P("chan", "blk", None),
        P("chan", None),
        P("chan", None),
        P("chan"),
        P(),
        P(),
        P(),
        P(),
    )
    out_specs = P("chan", "blk", None)
    return jax.shard_map(on_device, mesh=mesh, in_specs=in_specs, out_specs=out_specs, check_vma=False)
```
